128 devices in a mesh: grp: 4 (over x_hi, core), tile: 32 (over z, y, x_lo).
Axes of the slice: x: 4 (x_hi: 2, x_lo: 2; x = x_hi * 2 + x_lo), y: 4, z: 4, core: 2. Of those that a mesh axis runs over, the one named last changes fastest.
Arguments:
- factors: bfloat16 [4096, 128, 128], P('tile', 'grp'), may hold values from -0.09375 to 0.09375
- amplitudes: bfloat16 [2048, 128, 128], P('tile', 'grp'), may hold values from -6 to 6
- tile_mask: int32 [32, 2, 2], replicated, may hold values 0 or 1
Outputs:
- residual: bfloat16 [128, 64, 2048], P('tile', None, 'grp')
The draws below stay inside these ranges and needn't reach their ends.
All inputs are finite; a program needn't handle non-finite values.
Results may differ from the reference program's by a relative error of at most 0.011.
Values may be sent and summed in bfloat16 or wider, within the bound.
A program may use at most 128 MiB of HBM per device.

```python
import jax
import jax.numpy as jnp
from jax import lax

NAUX = 4096
NV = 128
VB = 64
NB = 64
IJB = 64
PAIRS = 2048
NVB = 2
NBLK = 32


def with_ends(drawn, key, least, high):
    longest = drawn.shape.index(max(drawn.shape))
    spots = []
    for shift in (0, 1):
        where = [jax.random.randint(jax.random.fold_in(key, axis), (), 0, length) for axis, length in enumerate(drawn.shape)]
        where[longest] = (where[longest] + shift) % drawn.shape[longest]
        spots.append(tuple(where))
    return drawn.at[spots[0]].set(least).at[spots[1]].set(high)


def block_levels(key, extent, cuts, low, high):
    loudness = 1.0
    for dim, parts in cuts:
        steps = jax.random.uniform(jax.random.fold_in(jax.random.fold_in(key, 6), dim), (parts,), jnp.float32, low / len(cuts), high / len(cuts))
        loudness = loudness * jnp.repeat(jnp.exp(steps), extent[dim] // parts).reshape((-1,) + (1,) * (len(extent) - 1 - dim))
    return loudness


def scatter_about(key, shape, width, most, cuts=(), kind=jnp.bfloat16):
    factor_of = block_levels(key, shape, cuts, -0.22, 0.18) if cuts else 1.0
    array = jax.random.normal(key, shape, jnp.float32) * width * factor_of
    return jnp.minimum(jnp.maximum(array, -most), most).astype(kind)


def setup_inputs(seed: int = 0) -> dict:
    splits = jax.random.split(jax.random.key(seed), 4)
    return {
        "factors": scatter_about(splits[0], (NAUX, NV, NV), NAUX ** -0.5, 0.09375, ((0, 32), (1, 4))),
        "amplitudes": scatter_about(splits[1], (PAIRS, NV, NV), 1.0, 6.0, ((0, 32), (1, 4))),
        "tile_mask": with_ends((jax.random.randint(splits[2], (NBLK, NVB, NVB), 0, 2) < 1).astype(jnp.int32), jax.random.fold_in(splits[2], 1), 0, 1),
    }


def reference(factors, amplitudes, tile_mask):
    block_width = 8
    pair_blocks = jnp.arange(PAIRS, dtype=jnp.int32) // IJB
    virt_blocks = jnp.arange(NV, dtype=jnp.int32) // VB
    by_pair = tile_mask[pair_blocks]
    amp_mask = by_pair[:, virt_blocks][:, :, virt_blocks].transpose(0, 2, 1)
    res_mask = by_pair[:, virt_blocks][:, :, virt_blocks[:NB]].transpose(1, 2, 0)
    screened = amplitudes * amp_mask.astype(jnp.bfloat16)
    window = factors[:, :, :NB].reshape(NAUX, NV * NB)

    def add_block(index, total):
        start = (index * block_width).astype(jnp.int32)
        left_part = lax.dynamic_slice_in_dim(factors, start, block_width, 1)
        left_part = left_part.reshape(NAUX, block_width * NV)
        gram = lax.dot_general(left_part, window, (((0,), (0,)), ((), ())), preferred_element_type=jnp.float32)
        integrals = gram.astype(jnp.bfloat16).reshape(block_width, NV, NV, NB).transpose(0, 2, 1, 3)
        integrals = integrals.reshape(block_width * NV, NV * NB)
        amps = lax.dynamic_slice_in_dim(screened, start, block_width, 2).transpose(0, 2, 1)
        amps = amps.reshape(PAIRS, block_width * NV)
        return total + jnp.dot(amps, integrals, preferred_element_type=jnp.float32)

    ladder = lax.fori_loop(0, NV // block_width, add_block, jnp.zeros((PAIRS, NV * NB), jnp.float32))
    ladder = ladder.reshape(PAIRS, NV, NB).transpose(1, 2, 0)
    return (ladder * res_mask.astype(jnp.float32)).astype(jnp.bfloat16)
```

```python
import functools

import jax
import jax.numpy as jnp
from jax import lax
from jax.experimental import pallas as pl
from jax.experimental.pallas import tpu as pltpu
from jax.sharding import PartitionSpec as P

MESH = pl.DeviceIdType.MESH
NB = 64
BF = jnp.bfloat16
F32 = jnp.float32


def remote(src, dst, send, recv, dev):
    return pltpu.make_async_remote_copy(
        src_ref=src, dst_ref=dst, send_sem=send, recv_sem=recv, device_id=dev, device_id_type=MESH
    )


class Gather:
    EVENTS = 18

    def __init__(self, piece, i, j, up, down, pair, send, recv, sibling=None):
        self.piece, self.i, self.j = piece, i, j
        self.up, self.down, self.pair = up, down, pair
        self.send, self.recv = send, recv
        self.sibling = sibling
        self.sent = []
        i1, i2, i3, o = lax.rem(i + 1, 4), lax.rem(i + 2, 4), lax.rem(i + 3, 4), 1 - j
        self.brings = [
            (i3, j, 0, None), (i1, j, 0, None), (i2, j, 0, 0), (i2, j, 0, 1),
            (i, o, 0, None), (i3, o, 0, None), (i1, o, 0, None), (i2, o, 0, 0), (i2, o, 0, 1),
            (i, o, 1, None),
            (i3, j, 1, None), (i1, j, 1, None), (i3, o, 1, None), (i1, o, 1, None),
            (i2, j, 1, 0), (i2, j, 1, 1), (i2, o, 1, 0), (i2, o, 1, 1),
        ]
        self.sends = [
            ((i, j, 0, None), up), ((i, j, 0, None), down), ((i3, j, 0, 0), up), ((i1, j, 0, 1), down),
            ((i, j, 0, None), pair), ((i3, j, 0, None), pair), ((i1, j, 0, None), pair), ((i2, j, 0, 0), pair), ((i2, j, 0, 1), pair),
            ((i, j, 1, None), pair),
            ((i, j, 1, None), up), ((i, j, 1, None), down), ((i, o, 1, None), up), ((i, o, 1, None), down),
            ((i3, j, 1, 0), up), ((i1, j, 1, 1), down), ((i3, o, 1, 0), up), ((i1, o, 1, 1), down),
        ]
        self.then = {0: (2, 5), 1: (3, 6), 2: (7,), 3: (8,), 9: (12, 13), 10: (14,), 11: (15,), 12: (16,), 13: (17,)}

    def _go(self, e):
        where, dev = self.sends[e]
        ref = self.piece(*where)
        copy = remote(ref, ref, self.send.at[e], self.recv.at[e], dev)
        copy.start()
        self.sent.append(copy)

    def _share(self, slot, where):
        if self.sibling is not None:
            dev, send, recv = self.sibling
            ref = self.piece(*where)
            copy = remote(ref, ref, send.at[slot], recv.at[slot], dev)
            copy.start()
            self.sent.append(copy)

    def begin(self, order=(9, 0, 1, 4, 10, 11)):
        for e in order:
            self._go(e)
        self._share(18, (self.i, self.j, 0, None))
        self._share(19, (self.i, self.j, 1, None))

    def event(self, e):
        ref = self.piece(*self.brings[e])
        remote(ref, ref, self.send.at[e], self.recv.at[e], self.pair).wait_recv()
        for s in self.then.get(e, ()):
            self._go(s)
        self._share(e, self.brings[e])

    def sibling_wait(self, other_piece):
        dev, send, recv = self.sibling
        for slot in range(20):
            where = self.brings[slot] if slot < 18 else (self.i, self.j, slot - 18, None)
            ref = other_piece(*where)
            remote(ref, ref, send.at[slot], recv.at[slot], dev).wait_recv()

    def finish(self):
        for copy in self.sent:
            copy.wait_send()


def kernel(
    fl, fr, tt, out,
    lb, rb, tb, gr, w, pb, rs,
    la_s, la_r, ra_s, ra_r, ta_s, ta_r,
    lg_s, lg_r, rg_s, rg_r, tg_s, tg_r,
    rd_s, rd_r, td_s, td_r, rs_s, rs_r,
):
    g, t = lax.axis_index("grp"), lax.axis_index("tile")
    xh, k = g // 2, lax.rem(g, 2)
    z, y, xl = t // 8, lax.rem(t // 2, 4), lax.rem(t, 2)
    v = lax.rem(xl + xh, 2)

    def dev(xh_, k_, z_, y_, xl_):
        return {"grp": xh_ * 2 + k_, "tile": z_ * 8 + y_ * 2 + xl_}

    yhi, ylo = y // 2, lax.rem(y, 2)
    routed = []
    for src, dst, ss, rr in ((fr, rb, ra_s, ra_r), (tt, tb, ta_s, ta_r)):
        for dl in range(2):
            y_to = 2 * k + dl

            @pl.when(y_to == y)
            def _():
                pltpu.make_async_copy(src.at[dl], dst.at[z, xl, y], rr.at[ylo]).start()

            @pl.when(y_to != y)
            def _():
                remote(src.at[dl], dst.at[z, xl, y], ss.at[dl], rr.at[ylo], dev(xh, yhi, z, y_to, xl)).start()

            routed.append((src, dst, ss, rr, dl, y_to))
    order = [(dz, dv, ac) for dz in (2, 1, 3, 0) for dv in (1, 0) for ac in (0, 1)]
    left = []
    for n, (dz, dv, ac) in enumerate(order):
        z_to, v_to, k_to = lax.rem(z + dz, 4), lax.rem(v + dv, 2), lax.rem(k + ac, 2)
        here = lb.at[xh, y, z, xl, k]
        if (dz, dv, ac) == (0, 0, 0):
            pltpu.make_async_copy(fl.at[z_to, v_to, k_to], here, la_r.at[n]).start()
        else:
            copy = remote(
                fl.at[z_to, v_to, k_to], here, la_s.at[n], la_r.at[n], dev(xh, k_to, z_to, y, lax.rem(xl + dv, 2))
            )
            copy.start()
            left.append(copy)

    def l_piece(i, j, part, half):
        if half is None:
            return lb.at[j, i, pl.ds(2 * part, 2)]
        return lb.at[j, i, 2 * part + half]

    def block_piece(buf, depth, core):
        def piece(i, j, part, half):
            if half is None:
                return buf.at[i, j, 2 * core + part]
            return buf.at[i, j, 2 * core + part, pl.ds(half * depth, depth)]

        return piece

    y_up, y_down = dev(xh, k, z, lax.rem(y + 1, 4), xl), dev(xh, k, z, lax.rem(y + 3, 4), xl)
    z_up, z_down = dev(xh, k, lax.rem(z + 1, 4), y, xl), dev(xh, k, lax.rem(z + 3, 4), y, xl)
    u_pair, v_pair = dev(1 - xh, k, z, y, 1 - xl), dev(xh, k, z, y, 1 - xl)
    sib = dev(xh, 1 - k, z, y, xl)
    lg = Gather(l_piece, y, xh, y_up, y_down, u_pair, lg_s, lg_r)
    rg = Gather(block_piece(rb, 4, k), z, xl, z_up, z_down, v_pair, rg_s, rg_r, (sib, rd_s, rd_r))
    tg = Gather(block_piece(tb, 8, k), z, xl, z_up, z_down, v_pair, tg_s, tg_r, (sib, td_s, td_r))

    def own_arrived(dst, ss, rr):
        for n in range(2):
            ref = dst.at[z, xl, 2 * k + n]
            remote(ref, ref, ss.at[n], rr.at[n], sib).wait_recv()

    own_arrived(rb, ra_s, ra_r)
    rg.begin()
    for n, (dz, dv, ac) in enumerate(order):
        ref = lb.at[xh, y, lax.rem(z - dz + 4, 4), lax.rem(xl + dv, 2), lax.rem(k + ac, 2)]
        remote(ref, ref, la_s.at[n], la_r.at[n], sib).wait_recv()
    lg.begin()
    own_arrived(tb, ta_s, ta_r)
    early, late = (9, 0, 1, 12, 13, 10, 11), (4, 5, 6, 2, 3, 14, 15, 7, 8, 16, 17)
    early = (9, 0, 1, 10, 11)
    late = (4, 12, 13, 5, 6, 2, 3, 14, 15, 16, 17, 7, 8)
    for e in early:
        rg.event(e)
        lg.event(e)
    tg.begin()
    for e in late:
        rg.event(e)
        lg.event(e)
    for e in early + late:
        tg.event(e)
    rg.sibling_wait(block_piece(rb, 4, 1 - k))
    tg.sibling_wait(block_piece(tb, 8, 1 - k))

    def gram(step, carry):
        n, h = step // 2, lax.rem(step, 2)
        for kc in range(2):
            total = jnp.zeros((256, 256), F32)
            for yy in range(4):
                lhs = jnp.concatenate([lb[h, yy, zz, x, kc] for zz in range(4) for x in range(2)], axis=1)
                rhs = jnp.concatenate(
                    [
                        jnp.concatenate([rb[zz, x, yy, 2 * n], rb[zz, x, yy, 2 * n + 1]], axis=1)
                        for zz in range(4)
                        for x in range(2)
                    ],
                    axis=0,
                )
                total = total + jnp.dot(lhs, rhs, preferred_element_type=F32)
            low = lax.broadcasted_iota(jnp.int32, (32, 128), 1) < 64
            for aa in range(4):
                for q in range(2):
                    x0 = total[aa * 64 : aa * 64 + 32, q * 128 : q * 128 + 128]
                    x1 = total[aa * 64 + 32 : aa * 64 + 64, q * 128 : q * 128 + 128]
                    y0 = jnp.where(low, x0, pltpu.roll(x1, 64, 1)).astype(BF)
                    y1 = jnp.where(low, pltpu.roll(x0, 64, 1), x1).astype(BF)
                    row = pl.multiple_of((2 * n + q) * 256 + h * 64 + kc * 32, 32)
                    w[pl.ds(row, 32), aa * 128 : aa * 128 + 128] = y0
                    w[pl.ds(row + 128, 32), aa * 128 : aa * 128 + 128] = y1
        return carry

    lax.fori_loop(0, 8, gram, 0)

    def ladder(step, carry):
        quarter, half = step // 2, lax.rem(step, 2)
        for m in range(2):
            lhs = jnp.concatenate(
                [
                    jnp.concatenate([tb[quarter, x, yy, dd] for dd in range(16)], axis=1)
                    for yy in (2 * m, 2 * m + 1)
                    for x in range(2)
                ],
                axis=0,
            )
            col = pl.multiple_of(half * 256, 256)
            got = jnp.dot(lhs, w[:, pl.ds(col, 256)], preferred_element_type=F32)
            pb[quarter, m * 256 : m * 256 + 256, pl.ds(col, 256)] = got.astype(BF)
        return carry

    lax.fori_loop(0, 8, ladder, 0)

    slot = v * 8 + xh * 4 + y
    mine = xl == k
    pieces = []
    for qt in range(4):
        for dy in (2, 1, 3, 0):
            ya = lax.rem(y + dy, 4)
            pi, ka = qt // 2, qt % 2
            src = pb.at[qt, :, pl.ds(pl.multiple_of(ya * 128, 128), 128)]
            n = qt * 4 + dy
            copy = remote(src, rs.at[slot], rs_s.at[n], rs_r.at[slot], dev(pi, ka, z, ya, k))
            if dy == 0:
                own = jnp.logical_and(mine, qt == g)

                @pl.when(own)
                def _():
                    pltpu.make_async_copy(src, rs.at[slot], rs_r.at[slot]).start()

                @pl.when(jnp.logical_not(own))
                def _():
                    copy.start()

                pieces.append((copy, jnp.logical_not(own)))
            else:
                copy.start()
                pieces.append((copy, None))

    for src, dst, ss, rr, dl, y_to in routed:

        @pl.when(y_to != y)
        def _():
            remote(src.at[dl], dst.at[z, xl, y], ss.at[dl], rr.at[ylo], sib).wait_send()

    for copy in left:
        copy.wait_send()
    lg.finish()
    rg.finish()
    tg.finish()

    for n in range(2):
        for m in range(8):
            ref = rs.at[n * 8 + m]
            remote(ref, ref, rs_s.at[0], rs_r.at[n * 8 + m], sib).wait_recv()
        total = rs[n * 8].astype(F32)
        for m in range(1, 8):
            total = total + rs[n * 8 + m].astype(F32)
        out[n * 128 : n * 128 + 128, :] = total.T.astype(BF)
    for copy, when in pieces:
        if when is None:
            copy.wait_send()
        else:

            @pl.when(when)
            def _():
                copy.wait_send()


def on_device(factors, amplitudes, tile_mask):
    g, t = lax.axis_index("grp"), lax.axis_index("tile")
    fl = factors.reshape(128, 32, 4, 4, 2, 2, 2).transpose(2, 5, 4, 3, 6, 1, 0).reshape(4, 2, 2, 256, 128)
    fr = factors[:, :, :NB].reshape(128, 2, 8, 2, NB).transpose(1, 2, 0, 3, 4).reshape(2, 8, 128, 128)
    amp_mask = jnp.repeat(tile_mask[t, :, g // 2], 64).astype(BF)
    screened = amplitudes * amp_mask[None, None, :]
    tt = screened.reshape(64, 2, 16, 128).transpose(1, 2, 0, 3)
    dma = pltpu.SemaphoreType.DMA
    any_space = pl.BlockSpec(memory_space=pl.ANY)
    result = pl.pallas_call(
        kernel,
        name="ladder",
        out_shape=jax.ShapeDtypeStruct((256, 512), BF),
        in_specs=[any_space] * 3,
        out_specs=pl.BlockSpec(memory_space=pltpu.VMEM),
        scratch_shapes=[
            pltpu.VMEM((2, 4, 4, 2, 2, 256, 128), BF),
            pltpu.VMEM((4, 2, 4, 8, 128, 128), BF),
            pltpu.VMEM((4, 2, 4, 16, 64, 128), BF),
            pltpu.VMEM((8, 128), F32),
            pltpu.VMEM((2048, 512), BF),
            pltpu.VMEM((4, 512, 512), BF),
            pltpu.VMEM((16, 512, 128), BF),
            dma((16,)), dma((16,)), dma((2,)), dma((2,)), dma((2,)), dma((2,)),
            dma((18,)), dma((18,)), dma((18,)), dma((18,)), dma((18,)), dma((18,)),
            dma((20,)), dma((20,)), dma((20,)), dma((20,)), dma((16,)), dma((16,)),
        ],
        compiler_params=pltpu.CompilerParams(has_side_effects=True, vmem_limit_bytes=60 * 1024 * 1024),
    )(fl, fr, tt)
    res_mask = jnp.repeat(lax.dynamic_slice(tile_mask[:, t // 16, 0], (g * 8,), (8,)), 64).astype(BF)
    return result.reshape(4, NB, 512) * res_mask[None, None, :]


def solution(mesh):
    placed = (P("tile", "grp", None), P("tile", "grp", None), P())
    return jax.shard_map(
        on_device, mesh=mesh, in_specs=placed, out_specs=P("tile", None, "grp"), check_vma=False
    )
```

```python
import functools

import jax
import jax.numpy as jnp
from jax import lax
from jax.experimental import pallas as pl
from jax.experimental.pallas import tpu as pltpu
from jax.sharding import PartitionSpec as P

MESH = pl.DeviceIdType.MESH
NB = 64
BF = jnp.bfloat16
F32 = jnp.float32
SUBS = [(dz, dv, ac) for dz, dv in ((0, 0), (1, 0), (3, 0), (0, 1), (1, 1), (3, 1), (2, 0), (2, 1)) for ac in (0, 1)]
SPANS = {(0, None): (0, 7), (0, 0): (0, 4), (0, 1): (4, 3), (1, None): (7, 9), (1, 0): (7, 4), (1, 1): (11, 5)}
PLAN = (
    "l4", "l0", "l1", "r4", "r0", "r1", "r9", "r10", "r11", "r3", "r2", "r5",
    "r13", "r12", "l9", "l10", "l11", "r6", "TB", "r14", "r15", "r8", "l3", "l2",
    "r7", "r16", "r17", "RS", "G00", "l5", "t0", "t1", "G10", "t4", "G03", "t10",
    "t11", "l13", "l12", "t2", "t3", "t9", "l6", "G01", "t5", "G13", "l14", "l15",
    "l8", "t14", "t15", "t12", "t13", "G11", "t6", "t7", "G02", "l7", "l16", "t8",
    "l17", "t16", "t17", "G12", "TS",
)


def remote(src, dst, send, recv, dev):
    return pltpu.make_async_remote_copy(
        src_ref=src, dst_ref=dst, send_sem=send, recv_sem=recv, device_id=dev, device_id_type=MESH
    )


class Gather:
    def __init__(self, name, piece, i, j, up, down, pair, send, recv, sibling=None):
        self.name, self.piece, self.i, self.j = name, piece, i, j
        self.pair = pair
        self.send, self.recv = send, recv
        self.sibling = sibling
        self.sent = []
        i1, i2, i3, o = lax.rem(i + 1, 4), lax.rem(i + 2, 4), lax.rem(i + 3, 4), 1 - j
        self.brings = [
            (i3, j, 0, None), (i1, j, 0, None), (i2, j, 0, 0), (i2, j, 0, 1),
            (i, o, 0, None), (i3, o, 0, None), (i1, o, 0, None), (i2, o, 0, 0), (i2, o, 0, 1),
            (i, o, 1, None),
            (i3, j, 1, None), (i1, j, 1, None), (i3, o, 1, None), (i1, o, 1, None),
            (i2, j, 1, 0), (i2, j, 1, 1), (i2, o, 1, 0), (i2, o, 1, 1),
        ]
        self.sends = [
            ((i, j, 0, None), up), ((i, j, 0, None), down), ((i3, j, 0, 0), up), ((i1, j, 0, 1), down),
            ((i, j, 0, None), pair), ((i3, j, 0, None), pair), ((i1, j, 0, None), pair), ((i2, j, 0, 0), pair), ((i2, j, 0, 1), pair),
            ((i, j, 1, None), pair),
            ((i, j, 1, None), up), ((i, j, 1, None), down), ((i, o, 1, None), up), ((i, o, 1, None), down),
            ((i3, j, 1, 0), up), ((i1, j, 1, 1), down), ((i3, o, 1, 0), up), ((i1, o, 1, 1), down),
        ]
        self.then = {0: (2, 5), 1: (3, 6), 2: (7,), 3: (8,), 9: (12, 13), 10: (14,), 11: (15,), 12: (16,), 13: (17,)}

    def _go(self, e):
        where, dev = self.sends[e]
        ref = self.piece(*where)
        copy = remote(ref, ref, self.send.at[e], self.recv.at[e], dev)
        copy.start()
        self.sent.append(copy)

    def _share(self, slot, where):
        if self.sibling is not None:
            dev, send, recv = self.sibling
            ref = self.piece(*where)
            copy = remote(ref, ref, send.at[slot], recv.at[slot], dev)
            copy.start()
            self.sent.append(copy)

    def begin(self, part):
        for e in ((0, 1, 4), (9, 10, 11))[part]:
            self._go(e)
        self._share(18 + part, (self.i, self.j, part, None))

    def event(self, e):
        with jax.named_scope(self.name + str(e)):
            ref = self.piece(*self.brings[e])
            remote(ref, ref, self.send.at[e], self.recv.at[e], self.pair).wait_recv()
            for s in self.then.get(e, ()):
                self._go(s)
            self._share(e, self.brings[e])

    def sibling_wait(self, other_piece):
        dev, send, recv = self.sibling
        with jax.named_scope(self.name + "_sib"):
            for slot in range(20):
                where = self.brings[slot] if slot < 18 else (self.i, self.j, slot - 18, None)
                ref = other_piece(*where)
                remote(ref, ref, send.at[slot], recv.at[slot], dev).wait_recv()

    def finish(self):
        for copy in self.sent:
            copy.wait_send()


def kernel(
    mask, fl, fr, tt, out,
    lb, rb, tb, gr, w, pb, rs,
    la_s, la_r, ra_s, ra_r, ta_s, ta_r,
    lg_s, lg_r, rg_s, rg_r, tg_s, tg_r,
    rd_s, rd_r, td_s, td_r, rs_s, rs_r,
):
    g, t = lax.axis_index("grp"), lax.axis_index("tile")
    xh, k = g // 2, lax.rem(g, 2)
    z, y, xl = t // 8, lax.rem(t // 2, 4), lax.rem(t, 2)
    v = lax.rem(xl + xh, 2)

    def dev(xh_, k_, z_, y_, xl_):
        return {"grp": xh_ * 2 + k_, "tile": z_ * 8 + y_ * 2 + xl_}

    barrier = pltpu.get_barrier_semaphore()
    with jax.named_scope("barrier"):
        count = 0
        for dz in range(4):
            for dy in range(4):
                for dh in range(2):
                    for dl in range(2):
                        for dk in range(2):
                            same_z = dz == 0
                            same_yh = dy == 0 and dh == 0
                            if (dz, dy, dh, dl, dk) == (0, 0, 0, 0, 0) or not (same_z or same_yh):
                                continue
                            pl.semaphore_signal(
                                barrier, inc=1,
                                device_id=dev(lax.rem(xh + dh, 2), lax.rem(k + dk, 2), lax.rem(z + dz, 4), lax.rem(y + dy, 4), lax.rem(xl + dl, 2)),
                                device_id_type=MESH,
                            )
                            count += 1
        pl.semaphore_wait(barrier, count)

    yhi, ylo = y // 2, lax.rem(y, 2)
    routed = []

    def route(src, dst, ss, rr, depth):
        for dl in range(2):
            y_to = 2 * k + dl
            here = dst.at[z, xl, pl.ds(y * depth, depth)]

            @pl.when(y_to == y)
            def _():
                pltpu.make_async_copy(src.at[dl], here, rr.at[ylo]).start()

            @pl.when(y_to != y)
            def _():
                remote(src.at[dl], here, ss.at[dl], rr.at[ylo], dev(xh, yhi, z, y_to, xl)).start()

            routed.append((src.at[dl], here, ss.at[dl], rr.at[ylo], y_to))

    left = []
    with jax.named_scope("issue"):
        for n, (dz, dv, ac) in enumerate(SUBS):
            z_to, v_to, k_to = lax.rem(z + dz, 4), lax.rem(v + dv, 2), lax.rem(k + ac, 2)
            src, here = fl.at[z_to, :, k_to, v_to], lb.at[xh, y, n]
            if n == 0:
                pltpu.make_async_copy(src, here, la_r.at[n]).start()
            else:
                copy = remote(src, here, la_s.at[n], la_r.at[n], dev(xh, k_to, z_to, y, lax.rem(xl + dv, 2)))
                copy.start()
                left.append(copy)
            if n == 3:
                route(fr, rb, ra_s, ra_r, 8)

    def l_piece(i, j, part, half):
        first, some = SPANS[part, half]
        return lb.at[j, i, pl.ds(first, some)]

    def block_piece(buf, scale, core):
        def piece(i, j, part, half):
            first, some = SPANS[part, half]
            return buf.at[i, j, pl.ds((core * 16 + first) * scale, some * scale)]

        return piece

    y_up, y_down = dev(xh, k, z, lax.rem(y + 1, 4), xl), dev(xh, k, z, lax.rem(y + 3, 4), xl)
    z_up, z_down = dev(xh, k, lax.rem(z + 1, 4), y, xl), dev(xh, k, lax.rem(z + 3, 4), y, xl)
    u_pair, v_pair = dev(1 - xh, k, z, y, 1 - xl), dev(xh, k, z, y, 1 - xl)
    sib = dev(xh, 1 - k, z, y, xl)
    lg = Gather("l", l_piece, y, xh, y_up, y_down, u_pair, lg_s, lg_r)
    rg = Gather("r", block_piece(rb, 1, k), z, xl, z_up, z_down, v_pair, rg_s, rg_r, (sib, rd_s, rd_r))
    tg = Gather("t", block_piece(tb, 2, k), z, xl, z_up, z_down, v_pair, tg_s, tg_r, (sib, td_s, td_r))

    def own_arrived(dst, ss, rr, depth, n):
        ref = dst.at[z, xl, pl.ds((2 * k + n) * depth, depth)]
        remote(ref, ref, ss.at[n], rr.at[n], sib).wait_recv()

    def left_arrived(n):
        ref = lb.at[xh, y, n]
        remote(ref, ref, la_s.at[n], la_r.at[n], sib).wait_recv()

    def gram(h_rel, dy, place):
        h, yy = lax.rem(xh + h_rel, 2), lax.rem(y + dy, 4)

        def step(n, carry):
            rhs = []
            for dz, dv, ac in SUBS[::2]:
                zz, x = lax.rem(z - dz + 4, 4), lax.rem(xl + xh + dv + h, 2)
                rhs.append(jnp.concatenate([rb[zz, x, yy * 8 + 2 * n], rb[zz, x, yy * 8 + 2 * n + 1]], axis=1))
            rhs = jnp.concatenate(rhs, axis=0)
            col = pl.ds(pl.multiple_of(n * 256, 256), 256)
            low = lax.broadcasted_iota(jnp.int32, (32, 128), 1) < 64
            for ac in range(2):
                lhs = jnp.concatenate([lb[h, yy, 2 * s + ac].reshape(256, 128) for s in range(8)], axis=1)
                got = jnp.dot(lhs, rhs, preferred_element_type=F32)
                if place != "first":
                    got = got + gr[h_rel, ac, :, col]
                if place != "last":
                    gr[h_rel, ac, :, col] = got
                    continue
                row = h * 64 + lax.rem(k + ac, 2) * 32
                for aa in range(4):
                    for q in range(2):
                        x0 = got[aa * 64 : aa * 64 + 32, q * 128 : q * 128 + 128]
                        x1 = got[aa * 64 + 32 : aa * 64 + 64, q * 128 : q * 128 + 128]
                        y0 = jnp.where(low, x0, pltpu.roll(x1, 64, 1)).astype(BF)
                        y1 = jnp.where(low, pltpu.roll(x0, 64, 1), x1).astype(BF)
                        at0 = pl.multiple_of((2 * n + q) * 256 + row, 32)
                        w[pl.ds(at0, 32), aa * 128 : aa * 128 + 128] = y0
                        w[pl.ds(at0 + 128, 32), aa * 128 : aa * 128 + 128] = y1
            return carry

        lax.fori_loop(0, 4, step, 0)

    with jax.named_scope("own_r"):
        own_arrived(rb, ra_s, ra_r, 8, 0)
        rg.begin(0)
        own_arrived(rb, ra_s, ra_r, 8, 1)
        rg.begin(1)
        route(tt, tb, ta_s, ta_r, 16)
    with jax.named_scope("own_l"):
        for n in range(7):
            left_arrived(n)
        lg.begin(0)
    with jax.named_scope("own_lb"):
        for n in range(7, 16):
            left_arrived(n)
        lg.begin(1)
    gathers = {"l": lg, "r": rg, "t": tg}
    for word in PLAN:
        if word == "TB":
            with jax.named_scope("own_t"):
                own_arrived(tb, ta_s, ta_r, 16, 0)
                tg.begin(0)
                own_arrived(tb, ta_s, ta_r, 16, 1)
                tg.begin(1)
        elif word == "RS":
            rg.sibling_wait(block_piece(rb, 1, 1 - k))
        elif word == "TS":
            tg.sibling_wait(block_piece(tb, 2, 1 - k))
        elif word[0] == "G":
            place = "last" if word[2] == "2" else "first" if word[2] == "0" else "more"
            with jax.named_scope(word):
                gram(int(word[1]), int(word[2]), place)
        else:
            gathers[word[0]].event(int(word[1:]))

    slot = v * 8 + xh * 4 + y
    mine = xl == k

    def piece(s, dy):
        qt = lax.rem(g + 1 + s, 4)
        ya = lax.rem(y + dy, 4)
        src = pb.at[qt, :, pl.ds(pl.multiple_of(ya * 128, 128), 128)]
        copy = remote(src, rs.at[slot], rs_s.at[s * 4 + dy], rs_r.at[slot], dev(qt // 2, lax.rem(qt, 2), z, ya, k))
        return src, copy

    def ladder(s, carry):
        qt = lax.rem(g + 1 + s, 4)
        low = lax.broadcasted_iota(jnp.int32, (1, 128), 1) < 64
        for m in range(2):
            lhs = []
            for yy in (2 * m, 2 * m + 1):
                for x in range(2):
                    block = (qt * 8 + yy * 2 + x) * 4 + xh
                    keep = jnp.where(low, mask[block], mask[block + 2]).astype(F32).astype(BF)
                    lhs.append(jnp.concatenate([tb[qt, x, yy * 16 + dd] * keep for dd in range(16)], axis=1))
            lhs = jnp.concatenate(lhs, axis=0)
            for half in range(2):
                got = jnp.dot(lhs, w[:, half * 256 : half * 256 + 256], preferred_element_type=F32)
                pb[qt, m * 256 : m * 256 + 256, half * 256 : half * 256 + 256] = got.astype(BF)
        for dy in (2, 1, 3, 0):
            src, copy = piece(s, dy)
            if dy == 0:
                own = jnp.logical_and(mine, s == 3)

                @pl.when(own)
                def _():
                    pltpu.make_async_copy(src, rs.at[slot], rs_r.at[slot]).start()

                @pl.when(jnp.logical_not(own))
                def _():
                    copy.start()

            else:
                copy.start()
        return carry

    with jax.named_scope("ladd"):
        lax.fori_loop(0, 4, ladder, 0)

    with jax.named_scope("drain"):
        for src, here, ss, rr, y_to in routed:

            @pl.when(y_to != y)
            def _():
                remote(src, here, ss, rr, sib).wait_send()

        for copy in left:
            copy.wait_send()
        lg.finish()
        rg.finish()
        tg.finish()

    for n in range(2):
        with jax.named_scope("rs%d" % n):
            for m in range(8):
                ref = rs.at[n * 8 + m]
                remote(ref, ref, rs_s.at[0], rs_r.at[n * 8 + m], sib).wait_recv()
        total = rs[n * 8].astype(F32)
        for m in range(1, 8):
            total = total + rs[n * 8 + m].astype(F32)
        total = total.T
        for m in range(8):
            keep = mask[(g * 8 + m) * 4 + (z // 2) * 2].astype(F32)
            out[n * 128 : n * 128 + 128, m * 64 : m * 64 + 64] = (total[:, m * 64 : m * 64 + 64] * keep).astype(BF)
    with jax.named_scope("drain2"):
        for s in range(4):
            for dy in range(4):
                _, copy = piece(s, dy)
                if (s, dy) == (3, 0):

                    @pl.when(jnp.logical_not(mine))
                    def _():
                        copy.wait_send()

                else:
                    copy.wait_send()


def on_device(factors, amplitudes, tile_mask):
    fl = factors.transpose(2, 1, 0).reshape(4, 4, 2, 2, 2, 32, 128)
    fr = factors[:, :, :NB].reshape(128, 2, 8, 2, NB).transpose(1, 2, 0, 3, 4).reshape(2, 8, 128, 128)
    tt = amplitudes.transpose(1, 0, 2).reshape(2, 16, 64, 128)
    dma = pltpu.SemaphoreType.DMA
    any_space = pl.BlockSpec(memory_space=pl.ANY)
    result = pl.pallas_call(
        kernel,
        name="ladder",
        out_shape=jax.ShapeDtypeStruct((256, 512), BF),
        in_specs=[pl.BlockSpec(memory_space=pltpu.SMEM)] + [any_space] * 3,
        out_specs=pl.BlockSpec(memory_space=pltpu.VMEM),
        scratch_shapes=[
            pltpu.VMEM((2, 4, 16, 4, 2, 32, 128), BF),
            pltpu.VMEM((4, 2, 32, 128, 128), BF),
            pltpu.VMEM((4, 2, 64, 64, 128), BF),
            pltpu.VMEM((2, 2, 256, 1024), F32),
            pltpu.VMEM((2048, 512), BF),
            pltpu.VMEM((4, 512, 512), BF),
            pltpu.VMEM((16, 512, 128), BF),
            dma((16,)), dma((16,)), dma((2,)), dma((2,)), dma((2,)), dma((2,)),
            dma((18,)), dma((18,)), dma((18,)), dma((18,)), dma((18,)), dma((18,)),
            dma((20,)), dma((20,)), dma((20,)), dma((20,)), dma((16,)), dma((16,)),
        ],
        compiler_params=pltpu.CompilerParams(
            collective_id=0, has_side_effects=True, vmem_limit_bytes=60 * 1024 * 1024
        ),
    )(tile_mask.reshape(128), fl, fr, tt)
    return result.reshape(4, NB, 512)


def solution(mesh):
    placed = (P("tile", "grp", None), P("tile", "grp", None), P())
    return jax.shard_map(
        on_device, mesh=mesh, in_specs=placed, out_specs=P("tile", None, "grp"), check_vma=False
    )
```

```python
import functools

import jax
import jax.numpy as jnp
from jax import lax
from jax.experimental import pallas as pl
from jax.experimental.pallas import tpu as pltpu
from jax.sharding import PartitionSpec as P

MESH = pl.DeviceIdType.MESH
NB = 64
BF = jnp.bfloat16
F32 = jnp.float32
SUBS = [(dz, dv, ac) for dz, dv in ((0, 0), (1, 0), (3, 0), (0, 1), (1, 1), (3, 1), (2, 0), (2, 1)) for ac in (0, 1)]
SPANS = {(0, None): (0, 7), (0, 0): (0, 4), (0, 1): (4, 3), (1, None): (7, 9), (1, 0): (7, 4), (1, 1): (11, 5)}
BLOCK_SPANS = {(0, None): (0, 7), (0, 0): (0, 2), (0, 1): (2, 5), (1, None): (7, 9), (1, 0): (7, 3), (1, 1): (10, 6)}
STEP = {0: 0, 1: 1, 3: 2}
PLAN = (
    "l4", "l0", "l1", "r4", "r0", "r1", "r9", "r10", "r11", "r3", "r2", "r5",
    "r13", "r12", "TB", "l9", "l10", "l11", "r6", "r14", "r15", "r8", "l3", "l2",
    "r7", "r16", "r17", "RS", "G00", "l5", "t0", "t1", "G10", "t4", "G03", "t10",
    "t11", "l13", "l12", "t2", "t3", "t9", "l6", "G01", "t5", "G13", "l14", "l15",
    "l8", "t14", "t15", "t12", "t13", "G11", "t6", "t7", "G02", "l7", "l16", "t8",
    "l17", "t16", "t17", "G12", "TS",
)


def remote(src, dst, send, recv, dev):
    return pltpu.make_async_remote_copy(
        src_ref=src, dst_ref=dst, send_sem=send, recv_sem=recv, device_id=dev, device_id_type=MESH
    )


class Gather:
    def __init__(self, name, piece, i, j, up, down, pair, send, recv, sibling=None):
        self.name, self.piece, self.i, self.j = name, piece, i, j
        self.pair = pair
        self.send, self.recv = send, recv
        self.sibling = sibling
        self.sent = []
        i1, i2, i3, o = lax.rem(i + 1, 4), lax.rem(i + 2, 4), lax.rem(i + 3, 4), 1 - j
        self.brings = [
            (i3, j, 0, None), (i1, j, 0, None), (i2, j, 0, 0), (i2, j, 0, 1),
            (i, o, 0, None), (i3, o, 0, None), (i1, o, 0, None), (i2, o, 0, 0), (i2, o, 0, 1),
            (i, o, 1, None),
            (i3, j, 1, None), (i1, j, 1, None), (i3, o, 1, None), (i1, o, 1, None),
            (i2, j, 1, 0), (i2, j, 1, 1), (i2, o, 1, 0), (i2, o, 1, 1),
        ]
        self.sends = [
            ((i, j, 0, None), up), ((i, j, 0, None), down), ((i3, j, 0, 0), up), ((i1, j, 0, 1), down),
            ((i, j, 0, None), pair), ((i3, j, 0, None), pair), ((i1, j, 0, None), pair), ((i2, j, 0, 0), pair), ((i2, j, 0, 1), pair),
            ((i, j, 1, None), pair),
            ((i, j, 1, None), up), ((i, j, 1, None), down), ((i, o, 1, None), up), ((i, o, 1, None), down),
            ((i3, j, 1, 0), up), ((i1, j, 1, 1), down), ((i3, o, 1, 0), up), ((i1, o, 1, 1), down),
        ]
        self.then = {0: (2, 5), 1: (3, 6), 2: (7,), 3: (8,), 9: (12, 13), 10: (14,), 11: (15,), 12: (16,), 13: (17,)}

    def _go(self, e):
        where, dev = self.sends[e]
        ref = self.piece(*where)
        copy = remote(ref, ref, self.send.at[e], self.recv.at[e], dev)
        copy.start()
        self.sent.append(copy)

    def _share(self, slot, where):
        if self.sibling is not None:
            dev, send, recv = self.sibling
            ref = self.piece(*where)
            copy = remote(ref, ref, send.at[slot], recv.at[slot], dev)
            copy.start()
            self.sent.append(copy)

    def begin(self, part):
        for e in ((0, 1, 4), (9, 10, 11))[part]:
            self._go(e)
        self._share(18 + part, (self.i, self.j, part, None))

    def event(self, e):
        with jax.named_scope(self.name + str(e)):
            ref = self.piece(*self.brings[e])
            remote(ref, ref, self.send.at[e], self.recv.at[e], self.pair).wait_recv()
            for s in self.then.get(e, ()):
                self._go(s)
            self._share(e, self.brings[e])

    def sibling_wait(self, other_piece):
        dev, send, recv = self.sibling
        with jax.named_scope(self.name + "_sib"):
            for slot in range(20):
                where = self.brings[slot] if slot < 18 else (self.i, self.j, slot - 18, None)
                ref = other_piece(*where)
                remote(ref, ref, send.at[slot], recv.at[slot], dev).wait_recv()

    def finish(self):
        for copy in self.sent:
            copy.wait_send()


def kernel(
    mask, fl, fr, tt, out,
    lb, rb, tb, gr, w, pb, m1, m2, rs,
    la_s, la_r, ra_s, ra_r, ta_s, ta_r,
    lg_s, lg_r, rg_s, rg_r, tg_s, tg_r,
    rd_s, rd_r, td_s, td_r, m1_s, m1_r, far_s, m2_r, near_s, rs_r,
):
    g, t = lax.axis_index("grp"), lax.axis_index("tile")
    xh, k = g // 2, lax.rem(g, 2)
    z, y, xl = t // 8, lax.rem(t // 2, 4), lax.rem(t, 2)
    v = lax.rem(xl + xh, 2)

    def dev(xh_, k_, z_, y_, xl_):
        return {"grp": xh_ * 2 + k_, "tile": z_ * 8 + y_ * 2 + xl_}

    barrier = pltpu.get_barrier_semaphore()
    with jax.named_scope("barrier"):
        count = 0
        for dz in range(4):
            for dy in range(4):
                for dh in range(2):
                    for dl in range(2):
                        for dk in range(2):
                            same_z = dz == 0
                            same_yh = dy == 0 and dh == 0
                            if (dz, dy, dh, dl, dk) == (0, 0, 0, 0, 0) or not (same_z or same_yh):
                                continue
                            pl.semaphore_signal(
                                barrier, inc=1,
                                device_id=dev(lax.rem(xh + dh, 2), lax.rem(k + dk, 2), lax.rem(z + dz, 4), lax.rem(y + dy, 4), lax.rem(xl + dl, 2)),
                                device_id_type=MESH,
                            )
                            count += 1
        pl.semaphore_wait(barrier, count)

    yhi, ylo = y // 2, lax.rem(y, 2)
    routed = []

    def route(src, dst, ss, rr, depth):
        for dl in range(2):
            y_to = 2 * k + dl
            here = dst.at[z, xl, pl.ds(y * depth, depth)]

            @pl.when(y_to == y)
            def _():
                pltpu.make_async_copy(src.at[dl], here, rr.at[ylo]).start()

            @pl.when(y_to != y)
            def _():
                remote(src.at[dl], here, ss.at[dl], rr.at[ylo], dev(xh, yhi, z, y_to, xl)).start()

            routed.append((src.at[dl], here, ss.at[dl], rr.at[ylo], y_to))

    left = []
    with jax.named_scope("issue"):
        for n, (dz, dv, ac) in enumerate(SUBS):
            z_to, v_to, k_to = lax.rem(z + dz, 4), lax.rem(v + dv, 2), lax.rem(k + ac, 2)
            src, here = fl.at[z_to, :, k_to, v_to], lb.at[xh, y, n]
            if n == 0:
                pltpu.make_async_copy(src, here, la_r.at[n]).start()
            else:
                copy = remote(src, here, la_s.at[n], la_r.at[n], dev(xh, k_to, z_to, y, lax.rem(xl + dv, 2)))
                copy.start()
                left.append(copy)
            if n == 3:
                route(fr, rb, ra_s, ra_r, 8)

    def l_piece(i, j, part, half):
        first, some = SPANS[part, half]
        return lb.at[j, i, pl.ds(first, some)]

    def block_piece(buf, scale, core):
        def piece(i, j, part, half):
            first, some = BLOCK_SPANS[part, half]
            return buf.at[i, j, pl.ds((core * 16 + first) * scale, some * scale)]

        return piece

    y_up, y_down = dev(xh, k, z, lax.rem(y + 1, 4), xl), dev(xh, k, z, lax.rem(y + 3, 4), xl)
    z_up, z_down = dev(xh, k, lax.rem(z + 1, 4), y, xl), dev(xh, k, lax.rem(z + 3, 4), y, xl)
    u_pair, v_pair = dev(1 - xh, k, z, y, 1 - xl), dev(xh, k, z, y, 1 - xl)
    sib = dev(xh, 1 - k, z, y, xl)
    lg = Gather("l", l_piece, y, xh, y_up, y_down, u_pair, lg_s, lg_r)
    rg = Gather("r", block_piece(rb, 1, k), z, xl, z_up, z_down, v_pair, rg_s, rg_r, (sib, rd_s, rd_r))
    tg = Gather("t", block_piece(tb, 2, k), z, xl, z_up, z_down, v_pair, tg_s, tg_r, (sib, td_s, td_r))

    def own_arrived(dst, ss, rr, depth, n):
        ref = dst.at[z, xl, pl.ds((2 * k + n) * depth, depth)]
        remote(ref, ref, ss.at[n], rr.at[n], sib).wait_recv()

    def left_arrived(n):
        ref = lb.at[xh, y, n]
        remote(ref, ref, la_s.at[n], la_r.at[n], sib).wait_recv()

    def gram(h_rel, dy, place):
        h, yy = lax.rem(xh + h_rel, 2), lax.rem(y + dy, 4)

        def step(n, carry):
            rhs = []
            for dz, dv, ac in SUBS[::2]:
                zz, x = lax.rem(z - dz + 4, 4), lax.rem(xl + xh + dv + h, 2)
                rhs.append(jnp.concatenate([rb[zz, x, yy * 8 + 2 * n], rb[zz, x, yy * 8 + 2 * n + 1]], axis=1))
            rhs = jnp.concatenate(rhs, axis=0)
            col = pl.ds(pl.multiple_of(n * 256, 256), 256)
            low = lax.broadcasted_iota(jnp.int32, (32, 128), 1) < 64
            for ac in range(2):
                lhs = jnp.concatenate([lb[h, yy, 2 * s + ac].reshape(256, 128) for s in range(8)], axis=1)
                got = jnp.dot(lhs, rhs, preferred_element_type=F32)
                if place != "first":
                    got = got + gr[h_rel, ac, :, col]
                if place != "last":
                    gr[h_rel, ac, :, col] = got
                    continue
                row = h * 64 + lax.rem(k + ac, 2) * 32
                for aa in range(4):
                    for q in range(2):
                        x0 = got[aa * 64 : aa * 64 + 32, q * 128 : q * 128 + 128]
                        x1 = got[aa * 64 + 32 : aa * 64 + 64, q * 128 : q * 128 + 128]
                        y0 = jnp.where(low, x0, pltpu.roll(x1, 64, 1)).astype(BF)
                        y1 = jnp.where(low, pltpu.roll(x0, 64, 1), x1).astype(BF)
                        at0 = pl.multiple_of((2 * n + q) * 256 + row, 32)
                        w[pl.ds(at0, 32), aa * 128 : aa * 128 + 128] = y0
                        w[pl.ds(at0 + 128, 32), aa * 128 : aa * 128 + 128] = y1
            return carry

        lax.fori_loop(0, 4, step, 0)

    with jax.named_scope("own_r"):
        own_arrived(rb, ra_s, ra_r, 8, 0)
        rg.begin(0)
        own_arrived(rb, ra_s, ra_r, 8, 1)
        rg.begin(1)
        route(tt, tb, ta_s, ta_r, 16)
    with jax.named_scope("own_l"):
        for n in range(7):
            left_arrived(n)
        lg.begin(0)
    with jax.named_scope("own_lb"):
        for n in range(7, 16):
            left_arrived(n)
        lg.begin(1)
    gathers = {"l": lg, "r": rg, "t": tg}
    for word in PLAN:
        if word == "TB":
            with jax.named_scope("own_t"):
                own_arrived(tb, ta_s, ta_r, 16, 0)
                tg.begin(0)
                own_arrived(tb, ta_s, ta_r, 16, 1)
                tg.begin(1)
        elif word == "RS":
            rg.sibling_wait(block_piece(rb, 1, 1 - k))
        elif word == "TS":
            tg.sibling_wait(block_piece(tb, 2, 1 - k))
        elif word[0] == "G":
            place = "last" if word[2] == "2" else "first" if word[2] == "0" else "more"
            with jax.named_scope(word):
                gram(int(word[1]), int(word[2]), place)
        else:
            gathers[word[0]].event(int(word[1:]))

    home = xl == k
    away = jnp.logical_not(home)

    def p_piece(pi, ka, e):
        ya = lax.rem(y + e, 4)
        return pb.at[2 * pi + ka, :, pl.ds(pl.multiple_of(ya * 128, 128), 128)]

    def cross(pi, ka):
        return remote(p_piece(pi, ka, 2), m1.at[ka, pi], m1_s.at[ka, pi], m1_r.at[ka, pi], (y_up, y_down)[ka])

    def to_pair(ka, e):
        n = ka * 3 + STEP[e]
        return remote(p_piece(1 - xh, ka, e), m2.at[n], far_s.at[n], m2_r.at[n], u_pair)

    def to_far(ka, e):
        n = ka * 3 + STEP[e]
        slot = 6 + STEP[e]
        owner = dev(1 - xh, ka, z, lax.rem(y + e, 4), 1 - xl)
        return remote(p_piece(1 - xh, ka, e), rs.at[slot], far_s.at[n], rs_r.at[slot], owner)

    def to_near(ka, e, kind):
        n = ka * 3 + STEP[e]
        slot = 3 * kind + STEP[e]
        owner = dev(xh, ka, z, lax.rem(y + e, 4), (xl, 1 - xl)[kind])
        return remote(p_piece(xh, ka, e), rs.at[slot], near_s.at[n], rs_r.at[slot], owner)

    def send_far(ka, e):
        @pl.when(home)
        def _():
            to_pair(ka, e).start()

        @pl.when(away)
        def _():
            to_far(ka, e).start()

    def send_home(ka, e):
        if e != 0:
            to_near(ka, e, 0).start()
            return

        @pl.when(k == ka)
        def _():
            pltpu.make_async_copy(p_piece(xh, ka, 0), rs.at[0], rs_r.at[0]).start()

        @pl.when(k != ka)
        def _():
            to_near(ka, 0, 0).start()

    def ladder(qt):
        low = lax.broadcasted_iota(jnp.int32, (1, 128), 1) < 64

        def rows(m, carry):
            lhs = []
            for yy in range(2):
                for x in range(2):
                    yyy = 2 * m + yy
                    block = qt * 8 + yyy * 2 + x
                    keep = jnp.where(low, mask[0, xh, block], mask[1, xh, block]).astype(F32).astype(BF)
                    lhs.append(jnp.concatenate([tb[qt, x, yyy * 16 + dd] * keep for dd in range(16)], axis=1))
            lhs = jnp.concatenate(lhs, axis=0)
            at = pl.ds(pl.multiple_of(m * 256, 256), 256)
            for half in range(2):
                got = jnp.dot(lhs, w[:, half * 256 : half * 256 + 256], preferred_element_type=F32)
                pb[qt, at, half * 256 : half * 256 + 256] = got.astype(BF)
            return carry

        lax.fori_loop(0, 2, rows, 0)

    def merge(pi, ka, e, other):
        ya = lax.rem(y + e, 4)
        at = pl.ds(pl.multiple_of(ya * 128, 128), 128)
        pb[2 * pi + ka, :, at] = (pb[2 * pi + ka, :, at].astype(F32) + other[...].astype(F32)).astype(BF)

    with jax.named_scope("ladd"):
        for pi, ka in ((1 - xh, 0), (1 - xh, 1), (xh, 0), (xh, 1)):
            ladder(2 * pi + ka)
            cross(pi, ka).start()
            for e in (0, (3, 1)[ka]):
                if pi is xh:

                    @pl.when(home)
                    def _():
                        send_home(ka, e)

                else:
                    send_far(ka, e)

    def take_cross(pi, ka):
        e = (1, 3)[ka]
        ref = m1.at[ka, pi]
        remote(ref, ref, m1_s.at[ka, pi], m1_r.at[ka, pi], sib).wait_recv()
        merge(pi, ka, e, ref)
        return e

    def take_pair(ka, e):
        n = ka * 3 + STEP[e]
        ref = m2.at[n]
        remote(ref, ref, far_s.at[n], m2_r.at[n], sib).wait_recv()
        merge(xh, ka, e, ref)
        to_near(ka, e, 1).start()

    with jax.named_scope("merge"):

        @pl.when(home)
        def _():
            for ka in range(2):
                to_pair(ka, take_cross(1 - xh, ka)).start()
            for ka in range(2):
                send_home(ka, take_cross(xh, ka))

        @pl.when(away)
        def _():
            take_pair(0, 0)
            take_pair(0, 3)
            for ka in range(2):
                to_far(ka, take_cross(1 - xh, ka)).start()
            take_pair(1, 0)
            take_pair(1, 1)
            for ka in range(2):
                take_cross(xh, ka)
            take_pair(0, 1)
            take_pair(1, 3)

    with jax.named_scope("drain"):
        for src, here, ss, rr, y_to in routed:

            @pl.when(y_to != y)
            def _():
                remote(src, here, ss, rr, sib).wait_send()

        for copy in left:
            copy.wait_send()
        lg.finish()
        rg.finish()
        tg.finish()

    def gathered(slots):
        total = None
        for n in slots:
            ref = rs.at[n]
            with jax.named_scope("rs%d" % n):
                remote(ref, ref, near_s.at[0], rs_r.at[n], sib).wait_recv()
            part = rs[n].astype(F32)
            total = part if total is None else total + part
        return total.T

    for half, slots in ((v, (0, 6, 1, 2, 7, 8)), (1 - v, (3, 4, 5))):
        total = gathered(slots)
        at = pl.ds(pl.multiple_of(half * 128, 128), 128)
        for m in range(8):
            keep = mask[z // 2, 0, g * 8 + m].astype(F32)
            out[at, m * 64 : m * 64 + 64] = (total[:, m * 64 : m * 64 + 64] * keep).astype(BF)
    with jax.named_scope("drain2"):
        for pi in range(2):
            for ka in range(2):
                cross(pi, ka).wait_send()
        for ka in range(2):
            for e in (0, 1, 3):
                to_pair(ka, e).wait_send()

        @pl.when(home)
        def _():
            for ka in range(2):
                for e in (1, 3):
                    to_near(ka, e, 0).wait_send()

                @pl.when(k != ka)
                def _():
                    to_near(ka, 0, 0).wait_send()

        @pl.when(away)
        def _():
            for ka in range(2):
                for e in (0, 1, 3):
                    to_near(ka, e, 1).wait_send()


def on_device(factors, amplitudes, tile_mask):
    fl = factors.transpose(2, 1, 0).reshape(4, 4, 2, 2, 2, 32, 128)
    fr = factors[:, :, :NB].reshape(128, 2, 8, 2, NB).transpose(1, 2, 0, 3, 4).reshape(2, 8, 128, 128)
    tt = amplitudes.transpose(1, 0, 2).reshape(2, 16, 64, 128)
    dma = pltpu.SemaphoreType.DMA
    any_space = pl.BlockSpec(memory_space=pl.ANY)
    result = pl.pallas_call(
        kernel,
        name="ladder",
        out_shape=jax.ShapeDtypeStruct((256, 512), BF),
        in_specs=[pl.BlockSpec(memory_space=pltpu.SMEM)] + [any_space] * 3,
        out_specs=pl.BlockSpec(memory_space=pltpu.VMEM),
        scratch_shapes=[
            pltpu.VMEM((2, 4, 16, 4, 2, 32, 128), BF),
            pltpu.VMEM((4, 2, 32, 128, 128), BF),
            pltpu.VMEM((4, 2, 64, 64, 128), BF),
            pltpu.VMEM((2, 2, 256, 1024), F32),
            pltpu.VMEM((2048, 512), BF),
            pltpu.VMEM((4, 512, 512), BF),
            pltpu.VMEM((2, 2, 512, 128), BF),
            pltpu.VMEM((6, 512, 128), BF),
            pltpu.VMEM((9, 512, 128), BF),
            dma((16,)), dma((16,)), dma((2,)), dma((2,)), dma((2,)), dma((2,)),
            dma((18,)), dma((18,)), dma((18,)), dma((18,)), dma((18,)), dma((18,)),
            dma((20,)), dma((20,)), dma((20,)), dma((20,)),
            dma((2, 2)), dma((2, 2)), dma((6,)), dma((6,)), dma((6,)), dma((9,)),
        ],
        compiler_params=pltpu.CompilerParams(
            collective_id=0, has_side_effects=True, vmem_limit_bytes=60 * 1024 * 1024
        ),
    )(tile_mask.transpose(1, 2, 0), fl, fr, tt)
    return result.reshape(4, NB, 512)


def solution(mesh):
    placed = (P("tile", "grp", None), P("tile", "grp", None), P())
    return jax.shard_map(
        on_device, mesh=mesh, in_specs=placed, out_specs=P("tile", None, "grp"), check_vma=False
    )
```

```python
import functools

import jax
import jax.numpy as jnp
from jax import lax
from jax.experimental import pallas as pl
from jax.experimental.pallas import tpu as pltpu
from jax.sharding import PartitionSpec as P

MESH = pl.DeviceIdType.MESH
NB = 64
BF = jnp.bfloat16
F32 = jnp.float32
SUBS = [(dz, dv, ac) for dz, dv in ((0, 0), (1, 0), (3, 0), (0, 1), (1, 1), (3, 1), (2, 0), (2, 1)) for ac in (0, 1)]
SPANS = {(0, None): (0, 7), (0, 0): (0, 4), (0, 1): (4, 3), (1, None): (7, 9), (1, 0): (7, 4), (1, 1): (11, 5)}
BLOCK_SPANS = {(0, None): (0, 7), (0, 0): (0, 4), (0, 1): (4, 3), (1, None): (7, 9), (1, 0): (7, 4), (1, 1): (11, 5)}
STEP = {0: 0, 1: 1, 3: 2}
PLAN = (
    "r0", "r1", "r9", "r4", "l4", "r10", "r11", "l0", "l1", "r3", "r2", "r5",
    "r12", "r13", "TB", "l9", "r14", "r15", "r6", "l10", "l11", "r8", "r7", "l3",
    "l2", "r16", "r17", "RS", "G00", "G10", "t0", "t1", "t9", "G03", "G01", "t4",
    "t10", "t11", "l5", "l13", "l12", "l6", "t2", "t3", "G13", "G11", "t13", "t12",
    "t5", "l14", "l15", "G02", "t6", "t14", "t15", "l8", "l7", "l16", "l17", "G12",
    "t7", "t8", "t16", "t17", "TS",
)


def remote(src, dst, send, recv, dev):
    return pltpu.make_async_remote_copy(
        src_ref=src, dst_ref=dst, send_sem=send, recv_sem=recv, device_id=dev, device_id_type=MESH
    )


class Gather:
    def __init__(self, name, piece, i, j, up, down, pair, send, recv, sibling=None):
        self.name, self.piece, self.i, self.j = name, piece, i, j
        self.pair = pair
        self.send, self.recv = send, recv
        self.sibling = sibling
        self.sent = []
        i1, i2, i3, o = lax.rem(i + 1, 4), lax.rem(i + 2, 4), lax.rem(i + 3, 4), 1 - j
        self.brings = [
            (i3, j, 0, None), (i1, j, 0, None), (i2, j, 0, 0), (i2, j, 0, 1),
            (i, o, 0, None), (i3, o, 0, None), (i1, o, 0, None), (i2, o, 0, 0), (i2, o, 0, 1),
            (i, o, 1, None),
            (i3, j, 1, None), (i1, j, 1, None), (i3, o, 1, None), (i1, o, 1, None),
            (i2, j, 1, 0), (i2, j, 1, 1), (i2, o, 1, 0), (i2, o, 1, 1),
        ]
        self.sends = [
            ((i, j, 0, None), up), ((i, j, 0, None), down), ((i3, j, 0, 0), up), ((i1, j, 0, 1), down),
            ((i, j, 0, None), pair), ((i3, j, 0, None), pair), ((i1, j, 0, None), pair), ((i2, j, 0, 0), pair), ((i2, j, 0, 1), pair),
            ((i, j, 1, None), pair),
            ((i, j, 1, None), up), ((i, j, 1, None), down), ((i, o, 1, None), up), ((i, o, 1, None), down),
            ((i3, j, 1, 0), up), ((i1, j, 1, 1), down), ((i3, o, 1, 0), up), ((i1, o, 1, 1), down),
        ]
        self.then = {0: (2, 5), 1: (3, 6), 2: (7,), 3: (8,), 9: (12, 13), 10: (14,), 11: (15,), 12: (16,), 13: (17,)}

    def _go(self, e):
        where, dev = self.sends[e]
        ref = self.piece(*where)
        copy = remote(ref, ref, self.send.at[e], self.recv.at[e], dev)
        copy.start()
        self.sent.append(copy)

    def _share(self, slot, where):
        if self.sibling is not None:
            dev, send, recv = self.sibling
            ref = self.piece(*where)
            copy = remote(ref, ref, send.at[slot], recv.at[slot], dev)
            copy.start()
            self.sent.append(copy)

    def begin(self, part):
        both = self.sibling is not None
        for e in ((0, 1) if both else (0, 1, 4), (9, 10, 11, 4) if both else (9, 10, 11))[part]:
            self._go(e)
        self._share(18 + part, (self.i, self.j, part, None))

    def event(self, e):
        with jax.named_scope(self.name + str(e)):
            ref = self.piece(*self.brings[e])
            remote(ref, ref, self.send.at[e], self.recv.at[e], self.pair).wait_recv()
            for s in self.then.get(e, ()):
                self._go(s)
            self._share(e, self.brings[e])

    def sibling_wait(self, other_piece):
        dev, send, recv = self.sibling
        with jax.named_scope(self.name + "_sib"):
            for slot in range(20):
                where = self.brings[slot] if slot < 18 else (self.i, self.j, slot - 18, None)
                ref = other_piece(*where)
                remote(ref, ref, send.at[slot], recv.at[slot], dev).wait_recv()

    def finish(self):
        for copy in self.sent:
            copy.wait_send()


def kernel(
    mask, fl, fr, tt, out,
    lb, rb, tb, gr, w, pb, m1, m2, rs,
    la_s, la_r, ra_s, ra_r, ta_s, ta_r,
    lg_s, lg_r, rg_s, rg_r, tg_s, tg_r,
    rd_s, rd_r, td_s, td_r, m1_s, m1_r, far_s, m2_r, near_s, rs_r,
):
    g, t = lax.axis_index("grp"), lax.axis_index("tile")
    xh, k = g // 2, lax.rem(g, 2)
    z, y, xl = t // 8, lax.rem(t // 2, 4), lax.rem(t, 2)
    v = lax.rem(xl + xh, 2)

    def dev(xh_, k_, z_, y_, xl_):
        return {"grp": xh_ * 2 + k_, "tile": z_ * 8 + y_ * 2 + xl_}

    barrier = pltpu.get_barrier_semaphore()
    with jax.named_scope("barrier"):
        count = 0
        for dz in range(4):
            for dy in range(4):
                for dh in range(2):
                    for dl in range(2):
                        for dk in range(2):
                            same_z = dz == 0
                            same_yh = dy == 0 and dh == 0
                            if (dz, dy, dh, dl, dk) == (0, 0, 0, 0, 0) or not (same_z or same_yh):
                                continue
                            pl.semaphore_signal(
                                barrier, inc=1,
                                device_id=dev(lax.rem(xh + dh, 2), lax.rem(k + dk, 2), lax.rem(z + dz, 4), lax.rem(y + dy, 4), lax.rem(xl + dl, 2)),
                                device_id_type=MESH,
                            )
                            count += 1
        pl.semaphore_wait(barrier, count)

    yhi, ylo = y // 2, lax.rem(y, 2)
    routed = []

    def route(src, dst, ss, rr, depth):
        for dl in range(2):
            y_to = 2 * k + dl
            here = dst.at[z, xl, pl.ds(y * depth, depth)]

            @pl.when(y_to == y)
            def _():
                pltpu.make_async_copy(src.at[dl], here, rr.at[ylo]).start()

            @pl.when(y_to != y)
            def _():
                remote(src.at[dl], here, ss.at[dl], rr.at[ylo], dev(xh, yhi, z, y_to, xl)).start()

            routed.append((src.at[dl], here, ss.at[dl], rr.at[ylo], y_to))

    left = []
    with jax.named_scope("issue"):
        for n, (dz, dv, ac) in enumerate(SUBS):
            z_to, v_to, k_to = lax.rem(z + dz, 4), lax.rem(v + dv, 2), lax.rem(k + ac, 2)
            src, here = fl.at[z_to, :, k_to, v_to], lb.at[xh, y, n]
            if n == 0:
                pltpu.make_async_copy(src, here, la_r.at[n]).start()
            else:
                copy = remote(src, here, la_s.at[n], la_r.at[n], dev(xh, k_to, z_to, y, lax.rem(xl + dv, 2)))
                copy.start()
                left.append(copy)
            if n == 3:
                route(fr, rb, ra_s, ra_r, 8)

    def l_piece(i, j, part, half):
        first, some = SPANS[part, half]
        return lb.at[j, i, pl.ds(first, some)]

    def block_piece(buf, scale, core):
        def piece(i, j, part, half):
            first, some = BLOCK_SPANS[part, half]
            return buf.at[i, j, pl.ds((core * 16 + first) * scale, some * scale)]

        return piece

    y_up, y_down = dev(xh, k, z, lax.rem(y + 1, 4), xl), dev(xh, k, z, lax.rem(y + 3, 4), xl)
    z_up, z_down = dev(xh, k, lax.rem(z + 1, 4), y, xl), dev(xh, k, lax.rem(z + 3, 4), y, xl)
    u_pair, v_pair = dev(1 - xh, k, z, y, 1 - xl), dev(xh, k, z, y, 1 - xl)
    sib = dev(xh, 1 - k, z, y, xl)
    lg = Gather("l", l_piece, y, xh, y_up, y_down, u_pair, lg_s, lg_r)
    rg = Gather("r", block_piece(rb, 1, k), z, xl, z_up, z_down, v_pair, rg_s, rg_r, (sib, rd_s, rd_r))
    tg = Gather("t", block_piece(tb, 2, k), z, xl, z_up, z_down, v_pair, tg_s, tg_r, (sib, td_s, td_r))

    def own_arrived(dst, ss, rr, depth, n):
        ref = dst.at[z, xl, pl.ds((2 * k + n) * depth, depth)]
        remote(ref, ref, ss.at[n], rr.at[n], sib).wait_recv()

    def left_arrived(n):
        ref = lb.at[xh, y, n]
        remote(ref, ref, la_s.at[n], la_r.at[n], sib).wait_recv()

    def gram(h_rel, dy, place):
        h, yy = lax.rem(xh + h_rel, 2), lax.rem(y + dy, 4)

        def step(n, carry):
            rhs = []
            for dz, dv, ac in SUBS[::2]:
                zz, x = lax.rem(z - dz + 4, 4), lax.rem(xl + xh + dv + h, 2)
                rhs.append(jnp.concatenate([rb[zz, x, yy * 8 + 2 * n], rb[zz, x, yy * 8 + 2 * n + 1]], axis=1))
            rhs = jnp.concatenate(rhs, axis=0)
            col = pl.ds(pl.multiple_of(n * 256, 256), 256)
            low = lax.broadcasted_iota(jnp.int32, (32, 128), 1) < 64
            for ac in range(2):
                lhs = jnp.concatenate([lb[h, yy, 2 * s + ac].reshape(256, 128) for s in range(8)], axis=1)
                got = jnp.dot(lhs, rhs, preferred_element_type=F32)
                if place != "first":
                    got = got + gr[h_rel, ac, :, col]
                if place != "last":
                    gr[h_rel, ac, :, col] = got
                    continue
                row = h * 64 + lax.rem(k + ac, 2) * 32
                for aa in range(4):
                    for q in range(2):
                        x0 = got[aa * 64 : aa * 64 + 32, q * 128 : q * 128 + 128]
                        x1 = got[aa * 64 + 32 : aa * 64 + 64, q * 128 : q * 128 + 128]
                        y0 = jnp.where(low, x0, pltpu.roll(x1, 64, 1)).astype(BF)
                        y1 = jnp.where(low, pltpu.roll(x0, 64, 1), x1).astype(BF)
                        at0 = pl.multiple_of((2 * n + q) * 256 + row, 32)
                        w[pl.ds(at0, 32), aa * 128 : aa * 128 + 128] = y0
                        w[pl.ds(at0 + 128, 32), aa * 128 : aa * 128 + 128] = y1
            return carry

        lax.fori_loop(0, 4, step, 0)

    with jax.named_scope("own_r"):
        own_arrived(rb, ra_s, ra_r, 8, 0)
        rg.begin(0)
        own_arrived(rb, ra_s, ra_r, 8, 1)
        rg.begin(1)
        route(tt, tb, ta_s, ta_r, 16)
    with jax.named_scope("own_l"):
        for n in range(7):
            left_arrived(n)
        lg.begin(0)
    with jax.named_scope("own_lb"):
        for n in range(7, 16):
            left_arrived(n)
        lg.begin(1)
    gathers = {"l": lg, "r": rg, "t": tg}
    for word in PLAN:
        if word == "TB":
            with jax.named_scope("own_t"):
                own_arrived(tb, ta_s, ta_r, 16, 0)
                tg.begin(0)
                own_arrived(tb, ta_s, ta_r, 16, 1)
                tg.begin(1)
        elif word == "RS":
            rg.sibling_wait(block_piece(rb, 1, 1 - k))
        elif word == "TS":
            tg.sibling_wait(block_piece(tb, 2, 1 - k))
        elif word[0] == "G":
            place = "last" if word[2] == "2" else "first" if word[2] == "0" else "more"
            with jax.named_scope(word):
                gram(int(word[1]), int(word[2]), place)
        else:
            gathers[word[0]].event(int(word[1:]))

    home = xl == k
    away = jnp.logical_not(home)

    def p_piece(pi, ka, e):
        ya = lax.rem(y + e, 4)
        return pb.at[2 * pi + ka, :, pl.ds(pl.multiple_of(ya * 128, 128), 128)]

    def cross(pi, ka):
        return remote(p_piece(pi, ka, 2), m1.at[ka, pi], m1_s.at[ka, pi], m1_r.at[ka, pi], (y_up, y_down)[ka])

    def to_pair(ka, e):
        n = ka * 3 + STEP[e]
        return remote(p_piece(1 - xh, ka, e), m2.at[n], far_s.at[n], m2_r.at[n], u_pair)

    def to_far(ka, e):
        n = ka * 3 + STEP[e]
        slot = 6 + STEP[e]
        owner = dev(1 - xh, ka, z, lax.rem(y + e, 4), 1 - xl)
        return remote(p_piece(1 - xh, ka, e), rs.at[slot], far_s.at[n], rs_r.at[slot], owner)

    def to_near(ka, e, kind):
        n = ka * 3 + STEP[e]
        slot = 3 * kind + STEP[e]
        owner = dev(xh, ka, z, lax.rem(y + e, 4), (xl, 1 - xl)[kind])
        return remote(p_piece(xh, ka, e), rs.at[slot], near_s.at[n], rs_r.at[slot], owner)

    def send_far(ka, e):
        @pl.when(home)
        def _():
            to_pair(ka, e).start()

        @pl.when(away)
        def _():
            to_far(ka, e).start()

    def send_home(ka, e):
        if e != 0:
            to_near(ka, e, 0).start()
            return

        @pl.when(k == ka)
        def _():
            pltpu.make_async_copy(p_piece(xh, ka, 0), rs.at[0], rs_r.at[0]).start()

        @pl.when(k != ka)
        def _():
            to_near(ka, 0, 0).start()

    def ladder(qt):
        low = lax.broadcasted_iota(jnp.int32, (1, 128), 1) < 64

        def rows(m, carry):
            lhs = []
            for yy in range(2):
                for x in range(2):
                    yyy = 2 * m + yy
                    block = qt * 8 + yyy * 2 + x
                    keep = jnp.where(low, mask[0, xh, block], mask[1, xh, block]).astype(F32).astype(BF)
                    lhs.append(jnp.concatenate([tb[qt, x, yyy * 16 + dd] * keep for dd in range(16)], axis=1))
            lhs = jnp.concatenate(lhs, axis=0)
            at = pl.ds(pl.multiple_of(m * 256, 256), 256)
            for half in range(2):
                got = jnp.dot(lhs, w[:, half * 256 : half * 256 + 256], preferred_element_type=F32)
                pb[qt, at, half * 256 : half * 256 + 256] = got.astype(BF)
            return carry

        lax.fori_loop(0, 2, rows, 0)

    def merge(pi, ka, e, other):
        ya = lax.rem(y + e, 4)
        at = pl.ds(pl.multiple_of(ya * 128, 128), 128)
        pb[2 * pi + ka, :, at] = (pb[2 * pi + ka, :, at].astype(F32) + other[...].astype(F32)).astype(BF)

    with jax.named_scope("ladd"):
        for pi, ka in ((1 - xh, 0), (1 - xh, 1), (xh, 0), (xh, 1)):
            ladder(2 * pi + ka)
            cross(pi, ka).start()
            for e in (0, (3, 1)[ka]):
                if pi is xh:

                    @pl.when(home)
                    def _():
                        send_home(ka, e)

                else:
                    send_far(ka, e)

    def take_cross(pi, ka):
        e = (1, 3)[ka]
        ref = m1.at[ka, pi]
        remote(ref, ref, m1_s.at[ka, pi], m1_r.at[ka, pi], sib).wait_recv()
        merge(pi, ka, e, ref)
        return e

    def take_pair(ka, e):
        n = ka * 3 + STEP[e]
        ref = m2.at[n]
        remote(ref, ref, far_s.at[n], m2_r.at[n], sib).wait_recv()
        merge(xh, ka, e, ref)
        to_near(ka, e, 1).start()

    with jax.named_scope("merge"):

        @pl.when(home)
        def _():
            for ka in range(2):
                to_pair(ka, take_cross(1 - xh, ka)).start()
            for ka in range(2):
                send_home(ka, take_cross(xh, ka))

        @pl.when(away)
        def _():
            take_pair(0, 0)
            take_pair(0, 3)
            for ka in range(2):
                to_far(ka, take_cross(1 - xh, ka)).start()
            take_pair(1, 0)
            take_pair(1, 1)
            for ka in range(2):
                take_cross(xh, ka)
            take_pair(0, 1)
            take_pair(1, 3)

    with jax.named_scope("drain"):
        for src, here, ss, rr, y_to in routed:

            @pl.when(y_to != y)
            def _():
                remote(src, here, ss, rr, sib).wait_send()

        for copy in left:
            copy.wait_send()
        lg.finish()
        rg.finish()
        tg.finish()

    def gathered(slots):
        total = None
        for n in slots:
            ref = rs.at[n]
            with jax.named_scope("rs%d" % n):
                remote(ref, ref, near_s.at[0], rs_r.at[n], sib).wait_recv()
            part = rs[n].astype(F32)
            total = part if total is None else total + part
        return total.T

    for half, slots in ((v, (0, 6, 1, 2, 7, 8)), (1 - v, (3, 4, 5))):
        total = gathered(slots)
        at = pl.ds(pl.multiple_of(half * 128, 128), 128)
        for m in range(8):
            keep = mask[z // 2, 0, g * 8 + m].astype(F32)
            out[at, m * 64 : m * 64 + 64] = (total[:, m * 64 : m * 64 + 64] * keep).astype(BF)
    with jax.named_scope("drain2"):
        for pi in range(2):
            for ka in range(2):
                cross(pi, ka).wait_send()
        for ka in range(2):
            for e in (0, 1, 3):
                to_pair(ka, e).wait_send()

        @pl.when(home)
        def _():
            for ka in range(2):
                for e in (1, 3):
                    to_near(ka, e, 0).wait_send()

                @pl.when(k != ka)
                def _():
                    to_near(ka, 0, 0).wait_send()

        @pl.when(away)
        def _():
            for ka in range(2):
                for e in (0, 1, 3):
                    to_near(ka, e, 1).wait_send()


def on_device(factors, amplitudes, tile_mask):
    fl = factors.transpose(2, 1, 0).reshape(4, 4, 2, 2, 2, 32, 128)
    fr = factors[:, :, :NB].reshape(128, 2, 8, 2, NB).transpose(1, 2, 0, 3, 4).reshape(2, 8, 128, 128)
    tt = amplitudes.transpose(1, 0, 2).reshape(2, 16, 64, 128)
    dma = pltpu.SemaphoreType.DMA
    any_space = pl.BlockSpec(memory_space=pl.ANY)
    result = pl.pallas_call(
        kernel,
        name="ladder",
        out_shape=jax.ShapeDtypeStruct((256, 512), BF),
        in_specs=[pl.BlockSpec(memory_space=pltpu.SMEM)] + [any_space] * 3,
        out_specs=pl.BlockSpec(memory_space=pltpu.VMEM),
        scratch_shapes=[
            pltpu.VMEM((2, 4, 16, 4, 2, 32, 128), BF),
            pltpu.VMEM((4, 2, 32, 128, 128), BF),
            pltpu.VMEM((4, 2, 64, 64, 128), BF),
            pltpu.VMEM((2, 2, 256, 1024), F32),
            pltpu.VMEM((2048, 512), BF),
            pltpu.VMEM((4, 512, 512), BF),
            pltpu.VMEM((2, 2, 512, 128), BF),
            pltpu.VMEM((6, 512, 128), BF),
            pltpu.VMEM((9, 512, 128), BF),
            dma((16,)), dma((16,)), dma((2,)), dma((2,)), dma((2,)), dma((2,)),
            dma((18,)), dma((18,)), dma((18,)), dma((18,)), dma((18,)), dma((18,)),
            dma((20,)), dma((20,)), dma((20,)), dma((20,)),
            dma((2, 2)), dma((2, 2)), dma((6,)), dma((6,)), dma((6,)), dma((9,)),
        ],
        compiler_params=pltpu.CompilerParams(
            collective_id=0, has_side_effects=True, vmem_limit_bytes=60 * 1024 * 1024
        ),
    )(tile_mask.transpose(1, 2, 0), fl, fr, tt)
    return result.reshape(4, NB, 512)


def solution(mesh):
    placed = (P("tile", "grp", None), P("tile", "grp", None), P())
    return jax.shard_map(
        on_device, mesh=mesh, in_specs=placed, out_specs=P("tile", None, "grp"), check_vma=False
    )
```

```python
import functools

import jax
import jax.numpy as jnp
from jax import lax
from jax.experimental import pallas as pl
from jax.experimental.pallas import tpu as pltpu
from jax.sharding import PartitionSpec as P

MESH = pl.DeviceIdType.MESH
NB = 64
BF = jnp.bfloat16
F32 = jnp.float32
VMEM_MIB = 48
SUBS = [(dz, dv, ac) for dz, dv in ((0, 0), (1, 0), (3, 0), (0, 1), (1, 1), (3, 1), (2, 0), (2, 1)) for ac in (0, 1)]
SPANS = {(0, None): (0, 8), (0, 0): (0, 4), (0, 1): (4, 4), (1, None): (8, 8), (1, 0): (8, 4), (1, 1): (12, 4)}
BLOCK_SPANS = {(0, None): (0, 7), (0, 0): (0, 4), (0, 1): (4, 3), (1, None): (7, 9), (1, 0): (7, 4), (1, 1): (11, 5)}
STEP = {0: 0, 1: 1, 3: 2}
PLAN = (
    "r0", "r1", "r9", "r4", "l4", "r10", "r11", "l0", "l1", "r3", "r2", "r5",
    "r12", "r13", "TB", "l9", "r14", "r15", "r6", "l10", "l11", "r8", "r7", "l3",
    "l2", "r16", "r17", "RS", "G00", "G10", "t0", "t1", "t9", "G03", "G01", "t4",
    "t10", "t11", "l5", "l13", "l12", "l6", "t2", "t3", "G13", "G11", "t13", "t12",
    "t5", "l14", "l15", "G02", "t6", "t14", "t15", "l8", "l7", "l16", "l17", "t7",
    "t8", "t16", "t17", "G12", "TS",
)


def remote(src, dst, send, recv, dev):
    return pltpu.make_async_remote_copy(
        src_ref=src, dst_ref=dst, send_sem=send, recv_sem=recv, device_id=dev, device_id_type=MESH
    )


class Gather:
    def __init__(self, name, piece, i, j, up, down, pair, send, recv, sibling=None):
        self.name, self.piece, self.i, self.j = name, piece, i, j
        self.pair = pair
        self.send, self.recv = send, recv
        self.sibling = sibling
        self.sent = []
        i1, i2, i3, o = lax.rem(i + 1, 4), lax.rem(i + 2, 4), lax.rem(i + 3, 4), 1 - j
        self.brings = [
            (i3, j, 0, None), (i1, j, 0, None), (i2, j, 0, 0), (i2, j, 0, 1),
            (i, o, 0, None), (i3, o, 0, None), (i1, o, 0, None), (i2, o, 0, 0), (i2, o, 0, 1),
            (i, o, 1, None),
            (i3, j, 1, None), (i1, j, 1, None), (i3, o, 1, None), (i1, o, 1, None),
            (i2, j, 1, 0), (i2, j, 1, 1), (i2, o, 1, 0), (i2, o, 1, 1),
        ]
        self.sends = [
            ((i, j, 0, None), up), ((i, j, 0, None), down), ((i3, j, 0, 0), up), ((i1, j, 0, 1), down),
            ((i, j, 0, None), pair), ((i3, j, 0, None), pair), ((i1, j, 0, None), pair), ((i2, j, 0, 0), pair), ((i2, j, 0, 1), pair),
            ((i, j, 1, None), pair),
            ((i, j, 1, None), up), ((i, j, 1, None), down), ((i, o, 1, None), up), ((i, o, 1, None), down),
            ((i3, j, 1, 0), up), ((i1, j, 1, 1), down), ((i3, o, 1, 0), up), ((i1, o, 1, 1), down),
        ]
        self.then = {0: (2, 5), 1: (3, 6), 2: (7,), 3: (8,), 9: (12, 13), 10: (14,), 11: (15,), 12: (16,), 13: (17,)}

    def _go(self, e):
        where, dev = self.sends[e]
        ref = self.piece(*where)
        copy = remote(ref, ref, self.send.at[e], self.recv.at[e], dev)
        copy.start()
        self.sent.append(copy)

    def _share(self, slot, where):
        if self.sibling is not None:
            dev, send, recv = self.sibling
            ref = self.piece(*where)
            copy = remote(ref, ref, send.at[slot], recv.at[slot], dev)
            copy.start()
            self.sent.append(copy)

    def begin(self, part):
        both = self.sibling is not None
        for e in ((0, 1) if both else (0, 1, 4), (9, 10, 11, 4) if both else (9, 10, 11))[part]:
            self._go(e)
        self._share(18 + part, (self.i, self.j, part, None))

    def event(self, e):
        with jax.named_scope(self.name + str(e)):
            ref = self.piece(*self.brings[e])
            remote(ref, ref, self.send.at[e], self.recv.at[e], self.pair).wait_recv()
            for s in self.then.get(e, ()):
                self._go(s)
            self._share(e, self.brings[e])

    def sibling_wait(self, other_piece):
        dev, send, recv = self.sibling
        with jax.named_scope(self.name + "_sib"):
            for slot in range(20):
                where = self.brings[slot] if slot < 18 else (self.i, self.j, slot - 18, None)
                ref = other_piece(*where)
                remote(ref, ref, send.at[slot], recv.at[slot], dev).wait_recv()

    def finish(self):
        for copy in self.sent:
            copy.wait_send()


def kernel(
    mask, fl, factors, amplitudes, out,
    lb, rb, tb, gr, w, pb, m1, m2, rs,
    f32s, t32s, fr, tt,
    la_s, la_r, ra_s, ra_r, ta_s, ta_r,
    lg_s, lg_r, rg_s, rg_r, tg_s, tg_r,
    rd_s, rd_r, td_s, td_r, m1_s, m1_r, far_s, m2_r, near_s, rs_r,
):
    g, t = lax.axis_index("grp"), lax.axis_index("tile")
    xh, k = g // 2, lax.rem(g, 2)
    z, y, xl = t // 8, lax.rem(t // 2, 4), lax.rem(t, 2)
    v = lax.rem(xl + xh, 2)

    def dev(xh_, k_, z_, y_, xl_):
        return {"grp": xh_ * 2 + k_, "tile": z_ * 8 + y_ * 2 + xl_}

    barrier = pltpu.get_barrier_semaphore()
    with jax.named_scope("barrier"):
        count = 0
        for dz in range(4):
            for dy in range(4):
                for dh in range(2):
                    for dl in range(2):
                        for dk in range(2):
                            same_z = dz == 0
                            same_yh = dy == 0 and dh == 0
                            if (dz, dy, dh, dl, dk) == (0, 0, 0, 0, 0) or not (same_z or same_yh):
                                continue
                            pl.semaphore_signal(
                                barrier, inc=1,
                                device_id=dev(lax.rem(xh + dh, 2), lax.rem(k + dk, 2), lax.rem(z + dz, 4), lax.rem(y + dy, 4), lax.rem(xl + dl, 2)),
                                device_id_type=MESH,
                            )
                            count += 1

    with jax.named_scope("prep_r"):
        low_q = lax.broadcasted_iota(jnp.int32, (128, 128), 1) < 64

        def widen(n, carry):
            rows = pl.ds(pl.multiple_of(n * 512, 512), 512)
            f32s[rows, :] = factors[pl.ds(n * 16, 16)].astype(F32).reshape(512, 128)
            return carry

        lax.fori_loop(0, 8, widen, 0)

        def pair_up(n, carry):
            even = f32s[pl.ds(2 * n, 128, stride=32), :]
            odd = f32s[pl.ds(2 * n + 1, 128, stride=32), :]
            fr[n] = jnp.where(low_q, even, pltpu.roll(odd, 64, 1)).astype(BF)
            return carry

        lax.fori_loop(0, 16, pair_up, 0)

    with jax.named_scope("barrier_wait"):
        pl.semaphore_wait(barrier, count)

    yhi, ylo = y // 2, lax.rem(y, 2)
    routed = []

    def route(src, dst, ss, rr, depth):
        for dl in range(2):
            y_to = 2 * k + dl
            here = dst.at[z, xl, pl.ds(y * depth, depth)]

            part = src.at[pl.ds(dl * depth, depth)]

            @pl.when(y_to == y)
            def _():
                pltpu.make_async_copy(part, here, rr.at[ylo]).start()

            @pl.when(y_to != y)
            def _():
                remote(part, here, ss.at[dl], rr.at[ylo], dev(xh, yhi, z, y_to, xl)).start()

            routed.append((part, here, ss.at[dl], rr.at[ylo], y_to))

    left = []
    with jax.named_scope("issue"):
        for n, (dz, dv, ac) in enumerate(SUBS):
            z_to, v_to, k_to = lax.rem(z + dz, 4), lax.rem(v + dv, 2), lax.rem(k + ac, 2)
            src, here = fl.at[z_to, :, k_to, v_to], lb.at[xh, y, n]
            if n == 0:
                pltpu.make_async_copy(src, here, la_r.at[n]).start()
            else:
                copy = remote(src, here, la_s.at[n], la_r.at[n], dev(xh, k_to, z_to, y, lax.rem(xl + dv, 2)))
                copy.start()
                left.append(copy)
            if n == 3:
                route(fr, rb, ra_s, ra_r, 8)

    def l_piece(i, j, part, half):
        first, some = SPANS[part, half]
        return lb.at[j, i, pl.ds(first, some)]

    def block_piece(buf, scale, core):
        def piece(i, j, part, half):
            first, some = BLOCK_SPANS[part, half]
            return buf.at[i, j, pl.ds((core * 16 + first) * scale, some * scale)]

        return piece

    y_up, y_down = dev(xh, k, z, lax.rem(y + 1, 4), xl), dev(xh, k, z, lax.rem(y + 3, 4), xl)
    z_up, z_down = dev(xh, k, lax.rem(z + 1, 4), y, xl), dev(xh, k, lax.rem(z + 3, 4), y, xl)
    u_pair, v_pair = dev(1 - xh, k, z, y, 1 - xl), dev(xh, k, z, y, 1 - xl)
    sib = dev(xh, 1 - k, z, y, xl)
    lg = Gather("l", l_piece, y, xh, y_up, y_down, u_pair, lg_s, lg_r)
    rg = Gather("r", block_piece(rb, 1, k), z, xl, z_up, z_down, v_pair, rg_s, rg_r, (sib, rd_s, rd_r))
    tg = Gather("t", block_piece(tb, 2, k), z, xl, z_up, z_down, v_pair, tg_s, tg_r, (sib, td_s, td_r))

    def own_arrived(dst, ss, rr, depth, n):
        ref = dst.at[z, xl, pl.ds((2 * k + n) * depth, depth)]
        remote(ref, ref, ss.at[n], rr.at[n], sib).wait_recv()

    def left_arrived(n):
        ref = lb.at[xh, y, n]
        remote(ref, ref, la_s.at[n], la_r.at[n], sib).wait_recv()

    def gram(h_rel, dy, place):
        h, yy = lax.rem(xh + h_rel, 2), lax.rem(y + dy, 4)

        def step(n, carry):
            rhs = []
            for dz, dv, ac in SUBS[::2]:
                zz, x = lax.rem(z - dz + 4, 4), lax.rem(xl + xh + dv + h, 2)
                rhs.append(jnp.concatenate([rb[zz, x, yy * 8 + 2 * n], rb[zz, x, yy * 8 + 2 * n + 1]], axis=1))
            rhs = jnp.concatenate(rhs, axis=0)
            col = pl.ds(pl.multiple_of(n * 256, 256), 256)
            low = lax.broadcasted_iota(jnp.int32, (32, 128), 1) < 64
            for ac in range(2):
                lhs = jnp.concatenate([lb[h, yy, 2 * s + ac].reshape(256, 128) for s in range(8)], axis=1)
                got = jnp.dot(lhs, rhs, preferred_element_type=F32)
                if place != "first":
                    got = got + gr[h_rel, ac, :, col]
                if place != "last":
                    gr[h_rel, ac, :, col] = got
                    continue
                row = h * 64 + lax.rem(k + ac, 2) * 32
                for aa in range(4):
                    for q in range(2):
                        x0 = got[aa * 64 : aa * 64 + 32, q * 128 : q * 128 + 128]
                        x1 = got[aa * 64 + 32 : aa * 64 + 64, q * 128 : q * 128 + 128]
                        y0 = jnp.where(low, x0, pltpu.roll(x1, 64, 1)).astype(BF)
                        y1 = jnp.where(low, pltpu.roll(x0, 64, 1), x1).astype(BF)
                        at0 = pl.multiple_of((2 * n + q) * 256 + row, 32)
                        w[pl.ds(at0, 32), aa * 128 : aa * 128 + 128] = y0
                        w[pl.ds(at0 + 128, 32), aa * 128 : aa * 128 + 128] = y1
            return carry

        lax.fori_loop(0, 4, step, 0)

    with jax.named_scope("prep_t"):
        for n in range(4):
            t32s[n * 512 : n * 512 + 512, :] = amplitudes[n * 16 : n * 16 + 16].astype(F32).reshape(512, 128)

        def major_d(n, carry):
            tt[n] = t32s[pl.ds(n, 64, stride=32), :].astype(BF)
            return carry

        lax.fori_loop(0, 32, major_d, 0)

    with jax.named_scope("own_r"):
        own_arrived(rb, ra_s, ra_r, 8, 0)
        rg.begin(0)
        own_arrived(rb, ra_s, ra_r, 8, 1)
        rg.begin(1)
        route(tt, tb, ta_s, ta_r, 16)
    with jax.named_scope("own_l"):
        for n in range(8):
            left_arrived(n)
        lg.begin(0)
    with jax.named_scope("own_lb"):
        for n in range(8, 16):
            left_arrived(n)
        lg.begin(1)
    gathers = {"l": lg, "r": rg, "t": tg}
    for word in PLAN:
        if word == "TB":
            with jax.named_scope("own_t"):
                own_arrived(tb, ta_s, ta_r, 16, 0)
                tg.begin(0)
                own_arrived(tb, ta_s, ta_r, 16, 1)
                tg.begin(1)
        elif word == "RS":
            rg.sibling_wait(block_piece(rb, 1, 1 - k))
        elif word == "TS":
            tg.sibling_wait(block_piece(tb, 2, 1 - k))
        elif word[0] == "G":
            place = "last" if word[2] == "2" else "first" if word[2] == "0" else "more"
            with jax.named_scope(word):
                gram(int(word[1]), int(word[2]), place)
        else:
            gathers[word[0]].event(int(word[1:]))

    home = xl == k
    away = jnp.logical_not(home)

    def p_piece(pi, ka, e):
        ya = lax.rem(y + e, 4)
        return pb.at[2 * pi + ka, :, pl.ds(pl.multiple_of(ya * 128, 128), 128)]

    def cross(pi, ka):
        return remote(p_piece(pi, ka, 2), m1.at[ka, pi], m1_s.at[ka, pi], m1_r.at[ka, pi], (y_up, y_down)[ka])

    def to_pair(ka, e):
        n = ka * 3 + STEP[e]
        return remote(p_piece(1 - xh, ka, e), m2.at[n], far_s.at[n], m2_r.at[n], u_pair)

    def to_far(ka, e):
        n = ka * 3 + STEP[e]
        slot = 6 + STEP[e]
        owner = dev(1 - xh, ka, z, lax.rem(y + e, 4), 1 - xl)
        return remote(p_piece(1 - xh, ka, e), rs.at[slot], far_s.at[n], rs_r.at[slot], owner)

    def to_near(ka, e, kind):
        n = ka * 3 + STEP[e]
        slot = 3 * kind + STEP[e]
        owner = dev(xh, ka, z, lax.rem(y + e, 4), (xl, 1 - xl)[kind])
        return remote(p_piece(xh, ka, e), rs.at[slot], near_s.at[n], rs_r.at[slot], owner)

    def send_far(ka, e):
        @pl.when(home)
        def _():
            to_pair(ka, e).start()

    def send_home(ka, e):
        if e != 0:
            to_near(ka, e, 0).start()
            return

        @pl.when(k == ka)
        def _():
            pltpu.make_async_copy(p_piece(xh, ka, 0), rs.at[0], rs_r.at[0]).start()

        @pl.when(k != ka)
        def _():
            to_near(ka, 0, 0).start()

    def ladder(qt):
        low = lax.broadcasted_iota(jnp.int32, (1, 128), 1) < 64

        def rows(m, carry):
            lhs = []
            for yy in range(2):
                for x in range(2):
                    yyy = 2 * m + yy
                    block = qt * 8 + yyy * 2 + x
                    keep = jnp.where(low, mask[0, xh, block], mask[1, xh, block]).astype(F32).astype(BF)
                    lhs.append(jnp.concatenate([tb[qt, x, yyy * 16 + dd] * keep for dd in range(16)], axis=1))
            lhs = jnp.concatenate(lhs, axis=0)
            at = pl.ds(pl.multiple_of(m * 256, 256), 256)
            for half in range(2):
                got = jnp.dot(lhs, w[:, half * 256 : half * 256 + 256], preferred_element_type=F32)
                pb[qt, at, half * 256 : half * 256 + 256] = got.astype(BF)
            return carry

        lax.fori_loop(0, 2, rows, 0)

    def merge(pi, ka, e, other):
        ya = lax.rem(y + e, 4)
        at = pl.ds(pl.multiple_of(ya * 128, 128), 128)
        pb[2 * pi + ka, :, at] = (pb[2 * pi + ka, :, at].astype(F32) + other[...].astype(F32)).astype(BF)

    with jax.named_scope("ladd"):
        for pi, ka in ((1 - xh, 0), (1 - xh, 1), (xh, 0), (xh, 1)):
            ladder(2 * pi + ka)
            cross(pi, ka).start()
            for e in (0, (3, 1)[ka]):
                if pi is xh:

                    @pl.when(home)
                    def _():
                        send_home(ka, e)

                else:
                    send_far(ka, e)

    def take_cross(pi, ka):
        e = (1, 3)[ka]
        ref = m1.at[ka, pi]
        remote(ref, ref, m1_s.at[ka, pi], m1_r.at[ka, pi], sib).wait_recv()
        merge(pi, ka, e, ref)
        return e

    def take_pair(ka, e):
        n = ka * 3 + STEP[e]
        ref = m2.at[n]
        remote(ref, ref, far_s.at[n], m2_r.at[n], sib).wait_recv()
        merge(xh, ka, e, ref)
        to_near(ka, e, 1).start()

    with jax.named_scope("merge"):

        @pl.when(home)
        def _():
            for ka in range(2):
                to_pair(ka, take_cross(1 - xh, ka)).start()
            for ka in range(2):
                send_home(ka, take_cross(xh, ka))

        @pl.when(away)
        def _():
            take_pair(0, 0)
            take_pair(0, 3)
            for ka, e in ((0, 0), (0, 3), (1, 0), (1, 1)):
                to_far(ka, e).start()
            for ka in range(2):
                to_far(ka, take_cross(1 - xh, ka)).start()
            take_pair(1, 0)
            take_pair(1, 1)
            for ka in range(2):
                take_cross(xh, ka)
            take_pair(0, 1)
            take_pair(1, 3)

    with jax.named_scope("drain"):
        for src, here, ss, rr, y_to in routed:

            @pl.when(y_to != y)
            def _():
                remote(src, here, ss, rr, sib).wait_send()

        for copy in left:
            copy.wait_send()
        lg.finish()
        rg.finish()
        tg.finish()

    def gathered(slots):
        total = None
        for n in slots:
            ref = rs.at[n]
            with jax.named_scope("rs%d" % n):
                remote(ref, ref, near_s.at[0], rs_r.at[n], sib).wait_recv()
            part = rs[n].astype(F32)
            total = part if total is None else total + part
        return total.T

    for half, slots in ((v, (0, 6, 1, 2, 7, 8)), (1 - v, (3, 4, 5))):
        total = gathered(slots)
        at = pl.ds(pl.multiple_of(half * 128, 128), 128)
        for m in range(8):
            keep = mask[z // 2, 0, g * 8 + m].astype(F32)
            out[at, m * 64 : m * 64 + 64] = (total[:, m * 64 : m * 64 + 64] * keep).astype(BF)
    with jax.named_scope("drain2"):
        for pi in range(2):
            for ka in range(2):
                cross(pi, ka).wait_send()
        for ka in range(2):
            for e in (0, 1, 3):
                to_pair(ka, e).wait_send()

        @pl.when(home)
        def _():
            for ka in range(2):
                for e in (1, 3):
                    to_near(ka, e, 0).wait_send()

                @pl.when(k != ka)
                def _():
                    to_near(ka, 0, 0).wait_send()

        @pl.when(away)
        def _():
            for ka in range(2):
                for e in (0, 1, 3):
                    to_near(ka, e, 1).wait_send()


def on_device(factors, amplitudes, tile_mask):
    fl = factors.transpose(2, 1, 0).reshape(4, 4, 2, 2, 2, 32, 128)
    dma = pltpu.SemaphoreType.DMA
    vmem_space = pl.BlockSpec(memory_space=pltpu.VMEM)
    result = pl.pallas_call(
        kernel,
        name="ladder",
        out_shape=jax.ShapeDtypeStruct((256, 512), BF),
        in_specs=[pl.BlockSpec(memory_space=pltpu.SMEM)] + [pl.BlockSpec(memory_space=pl.ANY), vmem_space, vmem_space],
        out_specs=vmem_space,
        scratch_shapes=[
            pltpu.VMEM((2, 4, 16, 4, 2, 32, 128), BF),
            pltpu.VMEM((4, 2, 32, 128, 128), BF),
            pltpu.VMEM((4, 2, 64, 64, 128), BF),
            pltpu.VMEM((2, 2, 256, 1024), F32),
            pltpu.VMEM((2048, 512), BF),
            pltpu.VMEM((4, 512, 512), BF),
            pltpu.VMEM((2, 2, 512, 128), BF),
            pltpu.VMEM((6, 512, 128), BF),
            pltpu.VMEM((9, 512, 128), BF),
            pltpu.VMEM((4096, 128), F32),
            pltpu.VMEM((2048, 128), F32),
            pltpu.VMEM((16, 128, 128), BF),
            pltpu.VMEM((32, 64, 128), BF),
            dma((16,)), dma((16,)), dma((2,)), dma((2,)), dma((2,)), dma((2,)),
            dma((18,)), dma((18,)), dma((18,)), dma((18,)), dma((18,)), dma((18,)),
            dma((20,)), dma((20,)), dma((20,)), dma((20,)),
            dma((2, 2)), dma((2, 2)), dma((6,)), dma((6,)), dma((6,)), dma((9,)),
        ],
        compiler_params=pltpu.CompilerParams(
            collective_id=0, has_side_effects=True, vmem_limit_bytes=VMEM_MIB * 1024 * 1024
        ),
    )(tile_mask.transpose(1, 2, 0), fl, factors, amplitudes)
    return result.reshape(4, NB, 512)


def solution(mesh):
    placed = (P("tile", "grp", None), P("tile", "grp", None), P())
    return jax.shard_map(
        on_device, mesh=mesh, in_specs=placed, out_specs=P("tile", None, "grp"), check_vma=False
    )
```

```python
import functools

import jax
import jax.numpy as jnp
from jax import lax
from jax.experimental import pallas as pl
from jax.experimental.pallas import tpu as pltpu
from jax.sharding import PartitionSpec as P

MESH = pl.DeviceIdType.MESH
NB = 64
BF = jnp.bfloat16
F32 = jnp.float32
VMEM_MIB = 48
SUBS = [(dz, dv, ac) for dz, dv in ((0, 0), (1, 0), (3, 0), (0, 1), (1, 1), (3, 1), (2, 0), (2, 1)) for ac in (0, 1)]
SPANS = {(0, None): (0, 7), (0, 0): (0, 4), (0, 1): (4, 3), (1, None): (7, 9), (1, 0): (7, 4), (1, 1): (11, 5)}
FIRST, PART = 4, 7
BLOCK_SPANS = {(0, None): (0, 7), (0, 0): (0, 4), (0, 1): (4, 3), (1, None): (7, 9), (1, 0): (7, 4), (1, 1): (11, 5)}
STEP = {0: 0, 1: 1, 3: 2}
PLAN = (
    "r0", "r1", "r9", "r4", "l18", "l4", "r10", "r11", "l0", "l1", "r3", "r2", "r5",
    "r12", "r13", "TB", "l9", "r14", "r15", "r6", "l10", "l11", "r8", "r7", "l3",
    "l2", "r16", "r17", "RS", "G00", "G10", "t0", "t1", "t9", "G03", "G01", "t4",
    "t10", "t11", "l5", "l13", "l12", "l6", "t2", "t3", "G13", "G11", "t13", "t12",
    "t5", "l14", "l15", "G02", "t6", "t14", "t15", "l8", "l7", "l16", "l17", "t7",
    "t8", "t16", "t17", "G12", "TS",
)


def remote(src, dst, send, recv, dev):
    return pltpu.make_async_remote_copy(
        src_ref=src, dst_ref=dst, send_sem=send, recv_sem=recv, device_id=dev, device_id_type=MESH
    )


class Gather:
    def __init__(self, name, piece, i, j, up, down, pair, send, recv, sibling=None):
        self.name, self.piece, self.i, self.j = name, piece, i, j
        self.pair = pair
        self.send, self.recv = send, recv
        self.sibling = sibling
        i1, i2, i3, o = lax.rem(i + 1, 4), lax.rem(i + 2, 4), lax.rem(i + 3, 4), 1 - j
        self.brings = [
            (i3, j, 0, None), (i1, j, 0, None), (i2, j, 0, 0), (i2, j, 0, 1),
            (i, o, 0, None), (i3, o, 0, None), (i1, o, 0, None), (i2, o, 0, 0), (i2, o, 0, 1),
            (i, o, 1, None),
            (i3, j, 1, None), (i1, j, 1, None), (i3, o, 1, None), (i1, o, 1, None),
            (i2, j, 1, 0), (i2, j, 1, 1), (i2, o, 1, 0), (i2, o, 1, 1),
        ]
        self.sends = [
            ((i, j, 0, None), up), ((i, j, 0, None), down), ((i3, j, 0, 0), up), ((i1, j, 0, 1), down),
            ((i, j, 0, None), pair), ((i3, j, 0, None), pair), ((i1, j, 0, None), pair), ((i2, j, 0, 0), pair), ((i2, j, 0, 1), pair),
            ((i, j, 1, None), pair),
            ((i, j, 1, None), up), ((i, j, 1, None), down), ((i, o, 1, None), up), ((i, o, 1, None), down),
            ((i3, j, 1, 0), up), ((i1, j, 1, 1), down), ((i3, o, 1, 0), up), ((i1, o, 1, 1), down),
        ]
        if sibling is None:
            self.brings[4], self.sends[4] = (i, o, 0, 1), ((i, j, 0, 1), pair)
            self.brings.append((i, o, 0, 0))
            self.sends.append(((i, j, 0, 0), pair))
        self.then = {0: (2, 5), 1: (3, 6), 2: (7,), 3: (8,), 9: (12, 13), 10: (14,), 11: (15,), 12: (16,), 13: (17,)}

    def _go(self, e):
        where, dev = self.sends[e]
        ref = self.piece(*where)
        remote(ref, ref, self.send.at[0], self.recv.at[e], dev).start()

    def _share(self, where):
        if self.sibling is not None:
            dev, send, recv = self.sibling
            ref = self.piece(*where)
            remote(ref, ref, send.at[0], recv.at[0], dev).start()

    def begin(self, part):
        both = self.sibling is not None
        for e in ((0, 1) if both else (0, 1, 4), (9, 10, 11, 4) if both else (9, 10, 11))[part]:
            self._go(e)
        self._share((self.i, self.j, part, None))

    def event(self, e):
        with jax.named_scope(self.name + str(e)):
            ref = self.piece(*self.brings[e])
            remote(ref, ref, self.send.at[0], self.recv.at[e], self.pair).wait_recv()
            for s in self.then.get(e, ()):
                self._go(s)
            self._share(self.brings[e])

    def sibling_wait(self, others):
        dev, send, recv = self.sibling
        with jax.named_scope(self.name + "_sib"):
            remote(others, others, send.at[0], recv.at[0], dev).wait_recv()

    def finish(self, seven, eight=None):
        remote(seven, seven, self.send.at[0], self.recv.at[0], self.pair).wait_send()
        if eight is not None:
            dev, send, recv = self.sibling
            remote(eight, eight, send.at[0], recv.at[0], dev).wait_send()


def kernel(
    mask, fl, factors, amplitudes, out,
    lb, rb, tb, gr, w, pb, m1, m2, rs,
    f32s, t32s, fr, tt,
    la_s, la_r, ra_s, ra_r, ta_s, ta_r,
    lg_s, lg_r, rg_s, rg_r, tg_s, tg_r,
    rd_s, rd_r, td_s, td_r, m1_s, m1_r, far_s, m2_r, near_s, rs_r,
):
    g, t = lax.axis_index("grp"), lax.axis_index("tile")
    xh, k = g // 2, lax.rem(g, 2)
    z, y, xl = t // 8, lax.rem(t // 2, 4), lax.rem(t, 2)
    v = lax.rem(xl + xh, 2)

    def dev(xh_, k_, z_, y_, xl_):
        return {"grp": xh_ * 2 + k_, "tile": z_ * 8 + y_ * 2 + xl_}

    barrier = pltpu.get_barrier_semaphore()
    with jax.named_scope("barrier"):
        count = 0
        for dz in range(4):
            for dy in range(4):
                for dh in range(2):
                    for dl in range(2):
                        for dk in range(2):
                            same_z = dz == 0
                            same_yh = dy == 0 and dh == 0
                            if (dz, dy, dh, dl, dk) == (0, 0, 0, 0, 0) or not (same_z or same_yh):
                                continue
                            pl.semaphore_signal(
                                barrier, inc=1,
                                device_id=dev(lax.rem(xh + dh, 2), lax.rem(k + dk, 2), lax.rem(z + dz, 4), lax.rem(y + dy, 4), lax.rem(xl + dl, 2)),
                                device_id_type=MESH,
                            )
                            count += 1

    with jax.named_scope("prep_r"):
        low_q = lax.broadcasted_iota(jnp.int32, (128, 128), 1) < 64

        def widen(n, carry):
            rows = pl.ds(pl.multiple_of(n * 512, 512), 512)
            f32s[rows, :] = factors[pl.ds(n * 16, 16)].astype(F32).reshape(512, 128)
            return carry

        lax.fori_loop(0, 8, widen, 0)

        def pair_up(n, carry):
            even = f32s[pl.ds(2 * n, 128, stride=32), :]
            odd = f32s[pl.ds(2 * n + 1, 128, stride=32), :]
            fr[n] = jnp.where(low_q, even, pltpu.roll(odd, 64, 1)).astype(BF)
            return carry

        lax.fori_loop(0, 16, pair_up, 0)

    with jax.named_scope("barrier_wait"):
        pl.semaphore_wait(barrier, count)

    yhi, ylo = y // 2, lax.rem(y, 2)
    routed = []

    def route(src, dst, ss, rr, depth):
        for dl in range(2):
            y_to = 2 * k + dl
            here = dst.at[z * 2 + xl, pl.ds(y * depth, depth)]

            part = src.at[pl.ds(dl * depth, depth)]

            @pl.when(y_to == y)
            def _():
                pltpu.make_async_copy(part, here, rr.at[ylo]).start()

            @pl.when(y_to != y)
            def _():
                remote(part, here, ss.at[dl], rr.at[ylo], dev(xh, yhi, z, y_to, xl)).start()

            routed.append((part, here, ss.at[dl], rr.at[ylo], y_to))

    with jax.named_scope("issue"):
        for n, (dz, dv, ac) in enumerate(SUBS):
            z_to, v_to, k_to = lax.rem(z + dz, 4), lax.rem(v + dv, 2), lax.rem(k + ac, 2)
            src, here = fl.at[z_to, :, k_to, v_to], lb.at[xh * 4 + y, n]
            if n == 0:
                pltpu.make_async_copy(src, here, la_r.at[0]).start()
            else:
                group = 0 if n < FIRST else 1 if n < PART else 2
                remote(src, here, la_s.at[0], la_r.at[group], dev(xh, k_to, z_to, y, lax.rem(xl + dv, 2))).start()
            if n == 3:
                route(fr, rb, ra_s, ra_r, 8)

    def l_piece(i, j, part, half):
        first, some = SPANS[part, half]
        return lb.at[j * 4 + i, pl.ds(first, some)]

    def block_piece(buf, scale, core):
        def piece(i, j, part, half):
            first, some = BLOCK_SPANS[part, half]
            return buf.at[i * 2 + j, pl.ds((core * 16 + first) * scale, some * scale)]

        return piece

    y_up, y_down = dev(xh, k, z, lax.rem(y + 1, 4), xl), dev(xh, k, z, lax.rem(y + 3, 4), xl)
    z_up, z_down = dev(xh, k, lax.rem(z + 1, 4), y, xl), dev(xh, k, lax.rem(z + 3, 4), y, xl)
    u_pair, v_pair = dev(1 - xh, k, z, y, 1 - xl), dev(xh, k, z, y, 1 - xl)
    sib = dev(xh, 1 - k, z, y, xl)
    lg = Gather("l", l_piece, y, xh, y_up, y_down, u_pair, lg_s, lg_r)
    rg = Gather("r", block_piece(rb, 1, k), z, xl, z_up, z_down, v_pair, rg_s, rg_r, (sib, rd_s, rd_r))
    tg = Gather("t", block_piece(tb, 2, k), z, xl, z_up, z_down, v_pair, tg_s, tg_r, (sib, td_s, td_r))

    def own_arrived(dst, ss, rr, depth, n):
        ref = dst.at[z * 2 + xl, pl.ds((2 * k + n) * depth, depth)]
        remote(ref, ref, ss.at[n], rr.at[n], sib).wait_recv()

    def left_arrived(group):
        first, last = ((0, FIRST), (FIRST, PART), (PART, 16))[group]
        ref = lb.at[xh * 4 + y, pl.ds(first, last - first)]
        remote(ref, ref, la_s.at[0], la_r.at[group], sib).wait_recv()

    def gram(h_rel, dy, place):
        h, yy = lax.rem(xh + h_rel, 2), lax.rem(y + dy, 4)

        def step(n, carry):
            rhs = []
            for dz, dv, ac in SUBS[::2]:
                zz, x = lax.rem(z - dz + 4, 4), lax.rem(xl + xh + dv + h, 2)
                rhs.append(jnp.concatenate([rb[zz * 2 + x, yy * 8 + 2 * n], rb[zz * 2 + x, yy * 8 + 2 * n + 1]], axis=1))
            rhs = jnp.concatenate(rhs, axis=0)
            col = pl.ds(pl.multiple_of(n * 256, 256), 256)
            low = lax.broadcasted_iota(jnp.int32, (32, 128), 1) < 64
            lhs = jnp.concatenate(
                [
                    jnp.concatenate([lb[h * 4 + yy, 2 * s + ac].reshape(256, 128) for s in range(8)], axis=1)
                    for ac in range(2)
                ],
                axis=0,
            )
            both = jnp.dot(lhs, rhs, preferred_element_type=F32)
            for ac in range(2):
                got = both[ac * 256 : ac * 256 + 256]
                if place != "first":
                    got = got + gr[h_rel, ac, :, col]
                if place != "last":
                    gr[h_rel, ac, :, col] = got
                    continue
                row = h * 64 + lax.rem(k + ac, 2) * 32
                for aa in range(4):
                    for q in range(2):
                        x0 = got[aa * 64 : aa * 64 + 32, q * 128 : q * 128 + 128]
                        x1 = got[aa * 64 + 32 : aa * 64 + 64, q * 128 : q * 128 + 128]
                        y0 = jnp.where(low, x0, pltpu.roll(x1, 64, 1)).astype(BF)
                        y1 = jnp.where(low, pltpu.roll(x0, 64, 1), x1).astype(BF)
                        at0 = pl.multiple_of((2 * n + q) * 256 + row, 32)
                        w[pl.ds(at0, 32), aa * 128 : aa * 128 + 128] = y0
                        w[pl.ds(at0 + 128, 32), aa * 128 : aa * 128 + 128] = y1
            return carry

        lax.fori_loop(0, 4, step, 0)

    with jax.named_scope("prep_t"):
        for n in range(4):
            t32s[n * 512 : n * 512 + 512, :] = amplitudes[n * 16 : n * 16 + 16].astype(F32).reshape(512, 128)

        def major_d(n, carry):
            tt[n] = t32s[pl.ds(n, 64, stride=32), :].astype(BF)
            return carry

        lax.fori_loop(0, 32, major_d, 0)

    with jax.named_scope("own_l"):
        left_arrived(0)
        lg._go(18)
    with jax.named_scope("own_l2"):
        left_arrived(1)
        lg.begin(0)
    with jax.named_scope("own_r"):
        own_arrived(rb, ra_s, ra_r, 8, 0)
        rg.begin(0)
        own_arrived(rb, ra_s, ra_r, 8, 1)
        rg.begin(1)
        route(tt, tb, ta_s, ta_r, 16)
    with jax.named_scope("own_lb"):
        left_arrived(2)
        lg.begin(1)
    gathers = {"l": lg, "r": rg, "t": tg}
    for word in PLAN:
        if word == "TB":
            with jax.named_scope("own_t"):
                own_arrived(tb, ta_s, ta_r, 16, 0)
                tg.begin(0)
                own_arrived(tb, ta_s, ta_r, 16, 1)
                tg.begin(1)
        elif word == "RS":
            rg.sibling_wait(rb.at[:, pl.ds((1 - k) * 16, 16)])
        elif word == "TS":
            tg.sibling_wait(tb.at[:, pl.ds((1 - k) * 32, 32)])
        elif word[0] == "G":
            place = "last" if word[2] == "2" else "first" if word[2] == "0" else "more"
            with jax.named_scope(word):
                gram(int(word[1]), int(word[2]), place)
        else:
            gathers[word[0]].event(int(word[1:]))

    home = xl == k
    away = jnp.logical_not(home)

    def p_piece(pi, ka, e):
        ya = lax.rem(y + e, 4)
        return pb.at[2 * pi + ka, :, pl.ds(pl.multiple_of(ya * 128, 128), 128)]

    def cross(pi, ka):
        return remote(p_piece(pi, ka, 2), m1.at[ka, pi], m1_s.at[ka, pi], m1_r.at[ka, pi], (y_up, y_down)[ka])

    def to_pair(ka, e):
        n = ka * 3 + STEP[e]
        return remote(p_piece(1 - xh, ka, e), m2.at[n], far_s.at[n], m2_r.at[n], u_pair)

    def to_far(ka, e):
        n = ka * 3 + STEP[e]
        slot = 6 + STEP[e]
        owner = dev(1 - xh, ka, z, lax.rem(y + e, 4), 1 - xl)
        return remote(p_piece(1 - xh, ka, e), rs.at[slot], far_s.at[n], rs_r.at[slot], owner)

    def to_near(ka, e, kind):
        n = ka * 3 + STEP[e]
        slot = 3 * kind + STEP[e]
        owner = dev(xh, ka, z, lax.rem(y + e, 4), (xl, 1 - xl)[kind])
        return remote(p_piece(xh, ka, e), rs.at[slot], near_s.at[n], rs_r.at[slot], owner)

    def send_far(ka, e):
        @pl.when(home)
        def _():
            to_pair(ka, e).start()

    def send_home(ka, e):
        if e != 0:
            to_near(ka, e, 0).start()
            return

        @pl.when(k == ka)
        def _():
            pltpu.make_async_copy(p_piece(xh, ka, 0), rs.at[0], rs_r.at[0]).start()

        @pl.when(k != ka)
        def _():
            to_near(ka, 0, 0).start()

    def ladder(qt):
        low = lax.broadcasted_iota(jnp.int32, (1, 128), 1) < 64

        def rows(half, carry):
            lhs = []
            for yyy in range(4):
                for x in range(2):
                    block = qt * 8 + yyy * 2 + x
                    keep = jnp.where(low, mask[0, xh, block], mask[1, xh, block]).astype(F32).astype(BF)
                    lhs.append(jnp.concatenate([tb[qt * 2 + x, yyy * 16 + dd] * keep for dd in range(16)], axis=1))
            lhs = jnp.concatenate(lhs, axis=0)
            at = pl.ds(pl.multiple_of(half * 256, 256), 256)
            pb[qt, :, at] = jnp.dot(lhs, w[:, at], preferred_element_type=F32).astype(BF)
            return carry

        lax.fori_loop(0, 2, rows, 0)

    def merge(pi, ka, e, other):
        ya = lax.rem(y + e, 4)
        at = pl.ds(pl.multiple_of(ya * 128, 128), 128)
        pb[2 * pi + ka, :, at] = (pb[2 * pi + ka, :, at].astype(F32) + other[...].astype(F32)).astype(BF)

    with jax.named_scope("ladd"):
        for pi, ka in ((1 - xh, 0), (1 - xh, 1), (xh, 0), (xh, 1)):
            ladder(2 * pi + ka)
            cross(pi, ka).start()
            for e in (0, (3, 1)[ka]):
                if pi is xh:

                    @pl.when(home)
                    def _():
                        send_home(ka, e)

                else:
                    send_far(ka, e)

    def take_cross(pi, ka):
        e = (1, 3)[ka]
        ref = m1.at[ka, pi]
        remote(ref, ref, m1_s.at[ka, pi], m1_r.at[ka, pi], sib).wait_recv()
        merge(pi, ka, e, ref)
        return e

    def take_pair(ka, e):
        n = ka * 3 + STEP[e]
        ref = m2.at[n]
        remote(ref, ref, far_s.at[n], m2_r.at[n], sib).wait_recv()
        merge(xh, ka, e, ref)
        to_near(ka, e, 1).start()

    with jax.named_scope("merge"):

        @pl.when(home)
        def _():
            for ka in range(2):
                to_pair(ka, take_cross(1 - xh, ka)).start()
            for ka in range(2):
                send_home(ka, take_cross(xh, ka))

        @pl.when(away)
        def _():
            take_pair(0, 0)
            take_pair(0, 3)
            for ka, e in ((0, 0), (0, 3), (1, 0), (1, 1)):
                to_far(ka, e).start()
            for ka in range(2):
                to_far(ka, take_cross(1 - xh, ka)).start()
            take_pair(1, 0)
            take_pair(1, 1)
            for ka in range(2):
                take_cross(xh, ka)
            take_pair(0, 1)
            take_pair(1, 3)

    with jax.named_scope("drain"):
        for src, here, ss, rr, y_to in routed:

            @pl.when(y_to != y)
            def _():
                remote(src, here, ss, rr, sib).wait_send()

        ref = lb.at[0, pl.ds(0, 15)]
        remote(ref, ref, la_s.at[0], la_r.at[0], sib).wait_send()
        lg.finish(lb.at[pl.ds(0, 7)])
        rg.finish(rb.at[pl.ds(0, 7), pl.ds(0, 16)], rb.at[:, pl.ds(0, 16)])
        tg.finish(tb.at[pl.ds(0, 7), pl.ds(0, 32)], tb.at[:, pl.ds(0, 32)])

    for half, slots in ((1 - v, (3, 4, 5)), (v, (0, 1, 2, 6, 7, 8))):
        for n in slots:
            ref = rs.at[n]
            with jax.named_scope("rs%d" % n):
                remote(ref, ref, near_s.at[0], rs_r.at[n], sib).wait_recv()

        def total(m, carry):
            cut = pl.ds(pl.multiple_of(m * 128, 128), 128)
            got = rs[slots[0], cut, :].astype(F32)
            for n in slots[1:]:
                got = got + rs[n, cut, :].astype(F32)
            block = g * 8 + 2 * m
            low = lax.broadcasted_iota(jnp.int32, (1, 128), 1) < 64
            keep = jnp.where(low, mask[z // 2, 0, block], mask[z // 2, 0, block + 1]).astype(F32)
            out[pl.ds(pl.multiple_of(half * 128, 128), 128), cut] = (got.T * keep).astype(BF)
            return carry

        lax.fori_loop(0, 4, total, 0)
    with jax.named_scope("drain2"):
        for pi in range(2):
            for ka in range(2):
                cross(pi, ka).wait_send()
        for ka in range(2):
            for e in (0, 1, 3):
                to_pair(ka, e).wait_send()

        @pl.when(home)
        def _():
            for ka in range(2):
                for e in (1, 3):
                    to_near(ka, e, 0).wait_send()

                @pl.when(k != ka)
                def _():
                    to_near(ka, 0, 0).wait_send()

        @pl.when(away)
        def _():
            for ka in range(2):
                for e in (0, 1, 3):
                    to_near(ka, e, 1).wait_send()


def on_device(factors, amplitudes, tile_mask):
    fl = factors.transpose(2, 1, 0).reshape(4, 4, 2, 2, 2, 32, 128)
    dma = pltpu.SemaphoreType.DMA
    vmem_space = pl.BlockSpec(memory_space=pltpu.VMEM)
    result = pl.pallas_call(
        kernel,
        name="ladder",
        out_shape=jax.ShapeDtypeStruct((256, 512), BF),
        in_specs=[pl.BlockSpec(memory_space=pltpu.SMEM)] + [pl.BlockSpec(memory_space=pl.ANY), vmem_space, vmem_space],
        out_specs=vmem_space,
        scratch_shapes=[
            pltpu.VMEM((8, 16, 4, 2, 32, 128), BF),
            pltpu.VMEM((8, 32, 128, 128), BF),
            pltpu.VMEM((8, 64, 64, 128), BF),
            pltpu.VMEM((2, 2, 256, 1024), F32),
            pltpu.VMEM((2048, 512), BF),
            pltpu.VMEM((4, 512, 512), BF),
            pltpu.VMEM((2, 2, 512, 128), BF),
            pltpu.VMEM((6, 512, 128), BF),
            pltpu.VMEM((9, 512, 128), BF),
            pltpu.VMEM((4096, 128), F32),
            pltpu.VMEM((2048, 128), F32),
            pltpu.VMEM((16, 128, 128), BF),
            pltpu.VMEM((32, 64, 128), BF),
            dma((1,)), dma((3,)), dma((2,)), dma((2,)), dma((2,)), dma((2,)),
            dma((1,)), dma((19,)), dma((1,)), dma((18,)), dma((1,)), dma((18,)),
            dma((1,)), dma((1,)), dma((1,)), dma((1,)),
            dma((2, 2)), dma((2, 2)), dma((6,)), dma((6,)), dma((6,)), dma((9,)),
        ],
        compiler_params=pltpu.CompilerParams(
            collective_id=0, has_side_effects=True, vmem_limit_bytes=VMEM_MIB * 1024 * 1024
        ),
    )(tile_mask.transpose(1, 2, 0), fl, factors, amplitudes)
    return result.reshape(4, NB, 512)


def solution(mesh):
    placed = (P("tile", "grp", None), P("tile", "grp", None), P())
    return jax.shard_map(
        on_device, mesh=mesh, in_specs=placed, out_specs=P("tile", None, "grp"), check_vma=False
    )
```

```python
import functools

import jax
import jax.numpy as jnp
from jax import lax
from jax.experimental import pallas as pl
from jax.experimental.pallas import tpu as pltpu
from jax.sharding import PartitionSpec as P

MESH = pl.DeviceIdType.MESH
NB = 64
BF = jnp.bfloat16
F32 = jnp.float32
VMEM_MIB = 48
SUBS = [(dz, dv, ac) for dz, dv in ((0, 0), (1, 0), (3, 0), (0, 1), (1, 1), (3, 1), (2, 0), (2, 1)) for ac in (0, 1)]
SPANS = {(0, None): (0, 7), (0, 0): (0, 4), (0, 1): (4, 3), (1, None): (7, 9), (1, 0): (7, 4), (1, 1): (11, 5)}
FIRST, PART = 4, 7
BLOCK_SPANS = {(0, None): (0, 7), (0, 0): (0, 4), (0, 1): (4, 3), (1, None): (7, 9), (1, 0): (7, 4), (1, 1): (11, 5)}
STEP = {0: 0, 1: 1, 3: 2}
PLAN = (
    "r0", "r1", "r9", "r4", "l18", "l4", "r10", "r11", "l0", "l1", "r3", "r2", "r5",
    "r12", "r13", "TB", "l9", "r14", "r15", "r6", "l10", "l11", "r8", "r7", "l3",
    "l2", "r16", "r17", "RS", "G00", "G10", "t0", "t1", "t9", "G03", "G01", "t4",
    "t10", "t11", "l5", "l13", "l12", "l6", "t2", "t3", "G13", "G11", "t13", "t12",
    "t5", "l14", "l15", "G02", "t6", "t14", "t15", "l8", "l7", "l16", "l17", "t7",
    "t8", "t16", "t17", "G12", "TS",
)


def remote(src, dst, send, recv, dev):
    return pltpu.make_async_remote_copy(
        src_ref=src, dst_ref=dst, send_sem=send, recv_sem=recv, device_id=dev, device_id_type=MESH
    )


class Gather:
    def __init__(self, name, piece, i, j, up, down, pair, send, recv, sibling=None):
        self.name, self.piece, self.i, self.j = name, piece, i, j
        self.pair = pair
        self.send, self.recv = send, recv
        self.sibling = sibling
        i1, i2, i3, o = lax.rem(i + 1, 4), lax.rem(i + 2, 4), lax.rem(i + 3, 4), 1 - j
        self.brings = [
            (i3, j, 0, None), (i1, j, 0, None), (i2, j, 0, 0), (i2, j, 0, 1),
            (i, o, 0, None), (i3, o, 0, None), (i1, o, 0, None), (i2, o, 0, 0), (i2, o, 0, 1),
            (i, o, 1, None),
            (i3, j, 1, None), (i1, j, 1, None), (i3, o, 1, None), (i1, o, 1, None),
            (i2, j, 1, 0), (i2, j, 1, 1), (i2, o, 1, 0), (i2, o, 1, 1),
        ]
        self.sends = [
            ((i, j, 0, None), up), ((i, j, 0, None), down), ((i3, j, 0, 0), up), ((i1, j, 0, 1), down),
            ((i, j, 0, None), pair), ((i3, j, 0, None), pair), ((i1, j, 0, None), pair), ((i2, j, 0, 0), pair), ((i2, j, 0, 1), pair),
            ((i, j, 1, None), pair),
            ((i, j, 1, None), up), ((i, j, 1, None), down), ((i, o, 1, None), up), ((i, o, 1, None), down),
            ((i3, j, 1, 0), up), ((i1, j, 1, 1), down), ((i3, o, 1, 0), up), ((i1, o, 1, 1), down),
        ]
        if sibling is None:
            self.brings[4], self.sends[4] = (i, o, 0, 1), ((i, j, 0, 1), pair)
            self.brings.append((i, o, 0, 0))
            self.sends.append(((i, j, 0, 0), pair))
        self.then = {0: (2, 5), 1: (3, 6), 2: (7,), 3: (8,), 9: (12, 13), 10: (14,), 11: (15,), 12: (16,), 13: (17,)}

    def _go(self, e):
        where, dev = self.sends[e]
        ref = self.piece(*where)
        remote(ref, ref, self.send.at[0], self.recv.at[e], dev).start()

    def _share(self, where):
        if self.sibling is not None:
            dev, send, recv = self.sibling
            ref = self.piece(*where)
            remote(ref, ref, send.at[0], recv.at[0], dev).start()

    def begin(self, part):
        both = self.sibling is not None
        for e in ((0, 1) if both else (0, 1, 4), (9, 10, 11, 4) if both else (9, 10, 11))[part]:
            self._go(e)
        self._share((self.i, self.j, part, None))

    def event(self, e):
        with jax.named_scope(self.name + str(e)):
            ref = self.piece(*self.brings[e])
            remote(ref, ref, self.send.at[0], self.recv.at[e], self.pair).wait_recv()
            for s in self.then.get(e, ()):
                self._go(s)
            self._share(self.brings[e])

    def sibling_wait(self, others):
        dev, send, recv = self.sibling
        with jax.named_scope(self.name + "_sib"):
            remote(others, others, send.at[0], recv.at[0], dev).wait_recv()

    def finish(self, seven, eight=None):
        remote(seven, seven, self.send.at[0], self.recv.at[0], self.pair).wait_send()
        if eight is not None:
            dev, send, recv = self.sibling
            remote(eight, eight, send.at[0], recv.at[0], dev).wait_send()


def kernel(
    mask, fl, factors, amplitudes, out,
    lb, rb, tb, gr, w, pb, m1, m2, rs,
    f32s, t32s, fr, tt,
    la_s, la_r, ra_s, ra_r, ta_s, ta_r,
    lg_s, lg_r, rg_s, rg_r, tg_s, tg_r,
    rd_s, rd_r, td_s, td_r, m1_s, m1_r, far_s, m2_r, near_s, rs_r,
):
    g, t = lax.axis_index("grp"), lax.axis_index("tile")
    xh, k = g // 2, lax.rem(g, 2)
    z, y, xl = t // 8, lax.rem(t // 2, 4), lax.rem(t, 2)
    v = lax.rem(xl + xh, 2)

    def dev(xh_, k_, z_, y_, xl_):
        return {"grp": xh_ * 2 + k_, "tile": z_ * 8 + y_ * 2 + xl_}

    barrier = pltpu.get_barrier_semaphore()
    with jax.named_scope("barrier"):
        count = 0
        for dz in range(4):
            for dy in range(4):
                for dh in range(2):
                    for dl in range(2):
                        for dk in range(2):
                            same_z = dz == 0
                            same_yh = dy == 0 and dh == 0
                            if (dz, dy, dh, dl, dk) == (0, 0, 0, 0, 0) or not (same_z or same_yh):
                                continue
                            pl.semaphore_signal(
                                barrier, inc=1,
                                device_id=dev(lax.rem(xh + dh, 2), lax.rem(k + dk, 2), lax.rem(z + dz, 4), lax.rem(y + dy, 4), lax.rem(xl + dl, 2)),
                                device_id_type=MESH,
                            )
                            count += 1

    with jax.named_scope("prep_r"):
        low_q = lax.broadcasted_iota(jnp.int32, (128, 128), 1) < 64

        def widen(n, carry):
            rows = pl.ds(pl.multiple_of(n * 512, 512), 512)
            f32s[rows, :] = factors[pl.ds(n * 16, 16)].astype(F32).reshape(512, 128)
            return carry

        lax.fori_loop(0, 8, widen, 0)

        def pair_up(n, carry):
            even = f32s[pl.ds(2 * n, 128, stride=32), :]
            odd = f32s[pl.ds(2 * n + 1, 128, stride=32), :]
            fr[n] = jnp.where(low_q, even, pltpu.roll(odd, 64, 1)).astype(BF)
            return carry

        lax.fori_loop(0, 16, pair_up, 0)

    with jax.named_scope("barrier_wait"):
        pl.semaphore_wait(barrier, count)

    yhi, ylo = y // 2, lax.rem(y, 2)
    routed = []

    def route(src, dst, ss, rr, depth):
        for dl in range(2):
            y_to = 2 * k + dl
            here = dst.at[z * 2 + xl, pl.ds(y * depth, depth)]

            part = src.at[pl.ds(dl * depth, depth)]

            @pl.when(y_to == y)
            def _():
                pltpu.make_async_copy(part, here, rr.at[ylo]).start()

            @pl.when(y_to != y)
            def _():
                remote(part, here, ss.at[dl], rr.at[ylo], dev(xh, yhi, z, y_to, xl)).start()

            routed.append((part, here, ss.at[dl], rr.at[ylo], y_to))

    with jax.named_scope("issue"):
        for n, (dz, dv, ac) in enumerate(SUBS):
            z_to, v_to, k_to = lax.rem(z + dz, 4), lax.rem(v + dv, 2), lax.rem(k + ac, 2)
            src, here = fl.at[z_to, :, k_to, v_to], lb.at[xh * 4 + y, n]
            if n == 0:
                pltpu.make_async_copy(src, here, la_r.at[0]).start()
            else:
                group = 0 if n < FIRST else 1 if n < PART else 2
                remote(src, here, la_s.at[0], la_r.at[group], dev(xh, k_to, z_to, y, lax.rem(xl + dv, 2))).start()
            if n == 3:
                route(fr, rb, ra_s, ra_r, 8)

    def l_piece(i, j, part, half):
        first, some = SPANS[part, half]
        return lb.at[j * 4 + i, pl.ds(first, some)]

    def block_piece(buf, scale, core):
        def piece(i, j, part, half):
            first, some = BLOCK_SPANS[part, half]
            return buf.at[i * 2 + j, pl.ds((core * 16 + first) * scale, some * scale)]

        return piece

    y_up, y_down = dev(xh, k, z, lax.rem(y + 1, 4), xl), dev(xh, k, z, lax.rem(y + 3, 4), xl)
    z_up, z_down = dev(xh, k, lax.rem(z + 1, 4), y, xl), dev(xh, k, lax.rem(z + 3, 4), y, xl)
    u_pair, v_pair = dev(1 - xh, k, z, y, 1 - xl), dev(xh, k, z, y, 1 - xl)
    sib = dev(xh, 1 - k, z, y, xl)
    lg = Gather("l", l_piece, y, xh, y_up, y_down, u_pair, lg_s, lg_r)
    rg = Gather("r", block_piece(rb, 1, k), z, xl, z_up, z_down, v_pair, rg_s, rg_r, (sib, rd_s, rd_r))
    tg = Gather("t", block_piece(tb, 2, k), z, xl, z_up, z_down, v_pair, tg_s, tg_r, (sib, td_s, td_r))

    def own_arrived(dst, ss, rr, depth, n):
        ref = dst.at[z * 2 + xl, pl.ds((2 * k + n) * depth, depth)]
        remote(ref, ref, ss.at[n], rr.at[n], sib).wait_recv()

    def left_arrived(group):
        first, last = ((0, FIRST), (FIRST, PART), (PART, 16))[group]
        ref = lb.at[xh * 4 + y, pl.ds(first, last - first)]
        remote(ref, ref, la_s.at[0], la_r.at[group], sib).wait_recv()

    def gram(h_rel, dy, place):
        h, yy = lax.rem(xh + h_rel, 2), lax.rem(y + dy, 4)

        def step(n, carry):
            rhs = []
            for dz, dv, ac in SUBS[::2]:
                zz, x = lax.rem(z - dz + 4, 4), lax.rem(xl + xh + dv + h, 2)
                rhs.append(jnp.concatenate([rb[zz * 2 + x, yy * 8 + 2 * n], rb[zz * 2 + x, yy * 8 + 2 * n + 1]], axis=1))
            rhs = jnp.concatenate(rhs, axis=0)
            col = pl.ds(pl.multiple_of(n * 256, 256), 256)
            low = lax.broadcasted_iota(jnp.int32, (32, 128), 1) < 64
            lhs = jnp.concatenate(
                [
                    jnp.concatenate([lb[h * 4 + yy, 2 * s + ac].reshape(256, 128) for s in range(8)], axis=1)
                    for ac in range(2)
                ],
                axis=0,
            )
            both = jnp.dot(lhs, rhs, preferred_element_type=F32)
            for ac in range(2):
                got = both[ac * 256 : ac * 256 + 256]
                if place != "first":
                    got = got + gr[h_rel, ac, :, col]
                if place != "last":
                    gr[h_rel, ac, :, col] = got
                    continue
                row = h * 64 + lax.rem(k + ac, 2) * 32
                for aa in range(4):
                    for q in range(2):
                        x0 = got[aa * 64 : aa * 64 + 32, q * 128 : q * 128 + 128]
                        x1 = got[aa * 64 + 32 : aa * 64 + 64, q * 128 : q * 128 + 128]
                        y0 = jnp.where(low, x0, pltpu.roll(x1, 64, 1)).astype(BF)
                        y1 = jnp.where(low, pltpu.roll(x0, 64, 1), x1).astype(BF)
                        at0 = pl.multiple_of((2 * n + q) * 256 + row, 32)
                        w[pl.ds(at0, 32), aa * 128 : aa * 128 + 128] = y0
                        w[pl.ds(at0 + 128, 32), aa * 128 : aa * 128 + 128] = y1
            return carry

        lax.fori_loop(0, 4, step, 0)

    with jax.named_scope("prep_t"):
        for n in range(4):
            t32s[n * 512 : n * 512 + 512, :] = amplitudes[n * 16 : n * 16 + 16].astype(F32).reshape(512, 128)

        def major_d(n, carry):
            tt[n] = t32s[pl.ds(n, 64, stride=32), :].astype(BF)
            return carry

        lax.fori_loop(0, 32, major_d, 0)

    with jax.named_scope("own_l"):
        left_arrived(0)
        lg._go(18)
    with jax.named_scope("own_l2"):
        left_arrived(1)
        lg.begin(0)
    with jax.named_scope("own_r"):
        own_arrived(rb, ra_s, ra_r, 8, 0)
        rg.begin(0)
        own_arrived(rb, ra_s, ra_r, 8, 1)
        rg.begin(1)
        route(tt, tb, ta_s, ta_r, 16)
    with jax.named_scope("own_lb"):
        left_arrived(2)
        lg.begin(1)
    gathers = {"l": lg, "r": rg, "t": tg}
    for word in PLAN:
        if word == "TB":
            with jax.named_scope("own_t"):
                own_arrived(tb, ta_s, ta_r, 16, 0)
                tg.begin(0)
                own_arrived(tb, ta_s, ta_r, 16, 1)
                tg.begin(1)
        elif word == "RS":
            rg.sibling_wait(rb.at[:, pl.ds((1 - k) * 16, 16)])
        elif word == "TS":
            tg.sibling_wait(tb.at[:, pl.ds((1 - k) * 32, 32)])
        elif word[0] == "G":
            place = "last" if word[2] == "2" else "first" if word[2] == "0" else "more"
            with jax.named_scope(word):
                gram(int(word[1]), int(word[2]), place)
        else:
            gathers[word[0]].event(int(word[1:]))

    home = xl == k
    away = jnp.logical_not(home)

    def p_piece(pi, ka, e):
        ya = lax.rem(y + e, 4)
        return pb.at[2 * pi + ka, :, pl.ds(pl.multiple_of(ya * 128, 128), 128)]

    def cross(pi, ka):
        return remote(p_piece(pi, ka, 2), m1.at[ka, pi], m1_s.at[0], m1_r.at[ka, pi], (y_up, y_down)[ka])

    def to_pair(ka, e):
        n = ka * 3 + STEP[e]
        return remote(p_piece(1 - xh, ka, e), m2.at[n], far_s.at[0], m2_r.at[n], u_pair)

    def to_far(ka, e):
        n = ka * 3 + STEP[e]
        slot = 6 + STEP[e]
        owner = dev(1 - xh, ka, z, lax.rem(y + e, 4), 1 - xl)
        return remote(p_piece(1 - xh, ka, e), rs.at[slot], far_s.at[0], rs_r.at[slot], owner)

    def to_near(ka, e, kind):
        n = ka * 3 + STEP[e]
        slot = 3 * kind + STEP[e]
        owner = dev(xh, ka, z, lax.rem(y + e, 4), (xl, 1 - xl)[kind])
        return remote(p_piece(xh, ka, e), rs.at[slot], near_s.at[0], rs_r.at[slot], owner)

    def send_far(ka, e):
        @pl.when(home)
        def _():
            to_pair(ka, e).start()

    def send_home(ka, e):
        if e != 0:
            to_near(ka, e, 0).start()
            return

        @pl.when(k == ka)
        def _():
            pltpu.make_async_copy(p_piece(xh, ka, 0), rs.at[0], rs_r.at[0]).start()

        @pl.when(k != ka)
        def _():
            to_near(ka, 0, 0).start()

    def ladder(qt):
        low = lax.broadcasted_iota(jnp.int32, (1, 128), 1) < 64

        def rows(half, carry):
            lhs = []
            for yyy in range(4):
                for x in range(2):
                    block = qt * 8 + yyy * 2 + x
                    keep = jnp.where(low, mask[0, xh, block], mask[1, xh, block]).astype(F32).astype(BF)
                    lhs.append(jnp.concatenate([tb[qt * 2 + x, yyy * 16 + dd] * keep for dd in range(16)], axis=1))
            lhs = jnp.concatenate(lhs, axis=0)
            at = pl.ds(pl.multiple_of(half * 256, 256), 256)
            pb[qt, :, at] = jnp.dot(lhs, w[:, at], preferred_element_type=F32).astype(BF)
            return carry

        lax.fori_loop(0, 2, rows, 0)

    def merge(pi, ka, e, other):
        ya = lax.rem(y + e, 4)
        at = pl.ds(pl.multiple_of(ya * 128, 128), 128)
        pb[2 * pi + ka, :, at] = (pb[2 * pi + ka, :, at].astype(F32) + other[...].astype(F32)).astype(BF)

    with jax.named_scope("ladd"):
        for pi, ka in ((1 - xh, 0), (1 - xh, 1), (xh, 0), (xh, 1)):
            ladder(2 * pi + ka)
            cross(pi, ka).start()
            for e in (0, (3, 1)[ka]):
                if pi is xh:

                    @pl.when(home)
                    def _():
                        send_home(ka, e)

                else:
                    send_far(ka, e)

    def take_cross(pi, ka):
        e = (1, 3)[ka]
        ref = m1.at[ka, pi]
        remote(ref, ref, m1_s.at[0], m1_r.at[ka, pi], sib).wait_recv()
        merge(pi, ka, e, ref)
        return e

    def take_pair(ka, e):
        n = ka * 3 + STEP[e]
        ref = m2.at[n]
        remote(ref, ref, far_s.at[0], m2_r.at[n], sib).wait_recv()
        merge(xh, ka, e, ref)
        to_near(ka, e, 1).start()

    with jax.named_scope("merge"):

        @pl.when(home)
        def _():
            for ka in range(2):
                to_pair(ka, take_cross(1 - xh, ka)).start()
            for ka in range(2):
                send_home(ka, take_cross(xh, ka))

        @pl.when(away)
        def _():
            take_pair(0, 0)
            take_pair(0, 3)
            for ka, e in ((0, 0), (0, 3), (1, 0), (1, 1)):
                to_far(ka, e).start()
            for ka in range(2):
                to_far(ka, take_cross(1 - xh, ka)).start()
            take_pair(1, 0)
            take_pair(1, 1)
            for ka in range(2):
                take_cross(xh, ka)
            take_pair(0, 1)
            take_pair(1, 3)

    with jax.named_scope("drain"):
        for src, here, ss, rr, y_to in routed:

            @pl.when(y_to != y)
            def _():
                remote(src, here, ss, rr, sib).wait_send()

        ref = lb.at[0, pl.ds(0, 15)]
        remote(ref, ref, la_s.at[0], la_r.at[0], sib).wait_send()
        lg.finish(lb.at[pl.ds(0, 7)])
        rg.finish(rb.at[pl.ds(0, 7), pl.ds(0, 16)], rb.at[:, pl.ds(0, 16)])
        tg.finish(tb.at[pl.ds(0, 7), pl.ds(0, 32)], tb.at[:, pl.ds(0, 32)])

    for half, slots in ((1 - v, (3, 4, 5)), (v, (0, 1, 2, 6, 7, 8))):
        for n in slots:
            ref = rs.at[n]
            with jax.named_scope("rs%d" % n):
                remote(ref, ref, near_s.at[0], rs_r.at[n], sib).wait_recv()

        def total(m, carry):
            cut = pl.ds(pl.multiple_of(m * 128, 128), 128)
            got = rs[slots[0], cut, :].astype(F32)
            for n in slots[1:]:
                got = got + rs[n, cut, :].astype(F32)
            block = g * 8 + 2 * m
            low = lax.broadcasted_iota(jnp.int32, (1, 128), 1) < 64
            keep = jnp.where(low, mask[z // 2, 0, block], mask[z // 2, 0, block + 1]).astype(F32)
            out[pl.ds(pl.multiple_of(half * 128, 128), 128), cut] = (got.T * keep).astype(BF)
            return carry

        lax.fori_loop(0, 4, total, 0)
    with jax.named_scope("drain2"):
        remote(m1, m1, m1_s.at[0], m1_r.at[0, 0], sib).wait_send()
        remote(m2, m2, far_s.at[0], m2_r.at[0], sib).wait_send()

        @pl.when(home)
        def _():
            five = rs.at[pl.ds(0, 5)]
            remote(five, five, near_s.at[0], rs_r.at[0], sib).wait_send()

        @pl.when(away)
        def _():
            six = rs.at[pl.ds(0, 6)]
            remote(six, six, near_s.at[0], rs_r.at[0], sib).wait_send()


def on_device(factors, amplitudes, tile_mask):
    fl = factors.transpose(2, 1, 0).reshape(4, 4, 2, 2, 2, 32, 128)
    dma = pltpu.SemaphoreType.DMA
    vmem_space = pl.BlockSpec(memory_space=pltpu.VMEM)
    result = pl.pallas_call(
        kernel,
        name="ladder",
        out_shape=jax.ShapeDtypeStruct((256, 512), BF),
        in_specs=[pl.BlockSpec(memory_space=pltpu.SMEM)] + [pl.BlockSpec(memory_space=pl.ANY), vmem_space, vmem_space],
        out_specs=vmem_space,
        scratch_shapes=[
            pltpu.VMEM((8, 16, 4, 2, 32, 128), BF),
            pltpu.VMEM((8, 32, 128, 128), BF),
            pltpu.VMEM((8, 64, 64, 128), BF),
            pltpu.VMEM((2, 2, 256, 1024), F32),
            pltpu.VMEM((2048, 512), BF),
            pltpu.VMEM((4, 512, 512), BF),
            pltpu.VMEM((2, 2, 512, 128), BF),
            pltpu.VMEM((6, 512, 128), BF),
            pltpu.VMEM((9, 512, 128), BF),
            pltpu.VMEM((4096, 128), F32),
            pltpu.VMEM((2048, 128), F32),
            pltpu.VMEM((16, 128, 128), BF),
            pltpu.VMEM((32, 64, 128), BF),
            dma((1,)), dma((3,)), dma((2,)), dma((2,)), dma((2,)), dma((2,)),
            dma((1,)), dma((19,)), dma((1,)), dma((18,)), dma((1,)), dma((18,)),
            dma((1,)), dma((1,)), dma((1,)), dma((1,)),
            dma((1,)), dma((2, 2)), dma((1,)), dma((6,)), dma((1,)), dma((9,)),
        ],
        compiler_params=pltpu.CompilerParams(
            collective_id=0, has_side_effects=True, vmem_limit_bytes=VMEM_MIB * 1024 * 1024
        ),
    )(tile_mask.transpose(1, 2, 0), fl, factors, amplitudes)
    return result.reshape(4, NB, 512)


def solution(mesh):
    placed = (P("tile", "grp", None), P("tile", "grp", None), P())
    return jax.shard_map(
        on_device, mesh=mesh, in_specs=placed, out_specs=P("tile", None, "grp"), check_vma=False
    )
```
